256 devices in a mesh: node: 64 (over z, x, core), freq: 4 (over y).
Axes of the slice: x: 4, y: 4, z: 8, core: 2. Of those that a mesh axis runs over, the one named last changes fastest.
Arguments:
- action_old: float32 [36, 36, 32768], P('freq', None, 'node'), may hold values from 0.05 to 2
- source: float32 [36, 36, 32768], P('freq', None, 'node'), may hold values from -4 to 4
- time_weight: float32 [32768], P('node'), may hold values from 0.5 to 4
- group_speed: float32 [36], P('freq'), may hold values from 0.3 to 3
- normals: float32 [2, 8, 32768], P(None, None, 'node'), may hold values from -3 to 3
- refract: float32 [32768], P('node'), may hold values from -4 to 4
- freq_shift: float32 [32768], P('node'), may hold values from -4 to 4
- nbr_list: int32 [64, 6], P('node'), may hold values from -1 to 63, as said below
- send_nodes: int32 [64, 6, 32], P('node'), may hold values from 0 to 511, as said below
- adjacency: int32 [8, 32768], P(None, 'node'), may hold values from 0 to 703, as said below
Outputs:
- action_new: float32 [36, 36, 32768], P('freq', None, 'node')
The draws below stay inside these ranges and needn't reach their ends.
Inputs may be any that keep to these rules, and one draw needn't show every extreme that they name: `nbr_list`: slot entries of subdomain p are distinct subdomains (p + o) or (p - o) modulo the number of subdomains, 1 <= o <= 3, or -1 for an empty slot; p + 1 and p - 1 are always listed; if p lists q then q lists p. `send_nodes`: local node indices of the sending subdomain. `adjacency`: entries as in the first step; an entry at or above 512 never names an empty slot.
All inputs are finite; a program needn't handle non-finite values.
Results may differ from the reference program's by a relative error of at most 0.000088.
Values sent between devices are 32-bit elements; how exact they have to be, the bound alone decides.
A program may use at most 128 MiB of HBM per device.

```python
import math
import jax
import jax.numpy as jnp

FREQ = 36
DIR = 36
ND = 512
DEG = 8
REACH = 3
ITERS = 3
NB = 6
H = 32
NODES = 32768
N_NODE = 64


def neighbour_table(key):
    base = jax.random.fold_in(key, 11)
    subdomain = jnp.arange(N_NODE)
    columns = []
    for reach in range(1, REACH + 1):
        if reach == 1:
            linked = jnp.ones((N_NODE,), jnp.int32)
        else:
            linked = jax.random.randint(jax.random.fold_in(base, reach), (N_NODE,), 0, 2)
        upward = jnp.where(linked > 0, (subdomain + reach) % N_NODE, -1)
        downward = jnp.where(jnp.roll(linked, reach) > 0, (subdomain - reach) % N_NODE, -1)
        columns.append(upward)
        columns.append(downward)
    candidates = jnp.stack(columns, axis=1)
    scores = jax.random.randint(jax.random.fold_in(base, 99), (N_NODE, NB), 0, 1 << 16) * NB + jnp.arange(NB)[None, :]
    order = jnp.argsort(scores, axis=1)
    return jnp.take_along_axis(candidates, order, axis=1).astype(jnp.int32)


def draw_nbr_list(key, part):
    return neighbour_table(key)


def draw_send_nodes(key, part):
    return jax.random.randint(jax.random.fold_in(key, 5), (N_NODE, NB, H), 0, ND).astype(jnp.int32)


def draw_adjacency(key, part):
    table = neighbour_table(key)
    degree = jax.random.randint(jax.random.fold_in(key, 21), (N_NODE, ND), 3, DEG + 1)
    own_index = jnp.arange(ND)
    nearby = (own_index[None, None, :] + jax.random.randint(jax.random.fold_in(key, 22), (DEG, N_NODE, ND), 1, ND)) % ND
    halo_pos = jax.random.randint(jax.random.fold_in(key, 23), (DEG, N_NODE, ND), 0, NB * H)
    slot_live = jnp.repeat(table >= 0, H, axis=1)
    halo_live = jnp.take_along_axis(jnp.broadcast_to(slot_live[None], (DEG, N_NODE, NB * H)), halo_pos, axis=2)
    use_halo = (jax.random.randint(jax.random.fold_in(key, 24), (DEG, N_NODE, ND), 0, 100) < 15) & halo_live
    entry = jnp.where(use_halo, ND + halo_pos, nearby)
    scores = jax.random.randint(jax.random.fold_in(key, 25), (N_NODE, ND), 0, 1 << 16) * ND + own_index[None, :]
    ranking = jnp.argsort(jnp.argsort(scores, axis=1), axis=1)
    covered = ranking < NB * H
    cover_pos = jnp.where(covered, ranking, 0)
    cover_live = covered & jnp.take_along_axis(slot_live, cover_pos, axis=1)
    first = jnp.where(cover_live, ND + cover_pos, entry[0])
    entry = entry.at[0].set(first)
    levels = jnp.arange(DEG)[:, None, None]
    entry = jnp.where(levels < degree[None], entry, own_index[None, None, :])
    return entry.reshape(DEG, N_NODE * ND).astype(jnp.int32)


def steps_of(stream_key, shape, split, smallest, high):
    def one(dim, parts):
        draws = jax.random.uniform(jax.random.fold_in(jax.random.fold_in(stream_key, 6), dim), (parts,), jnp.float32, smallest / len(split), high / len(split))
        return jnp.repeat(jnp.exp(draws), shape[dim] // parts).reshape((-1,) + (1,) * (len(shape) - dim - 1))

    factor_of = one(*split[0])
    for cut in split[1:]:
        factor_of = factor_of * one(*cut)
    return factor_of


def scatter_about(own_key, extent, deviation, bound, cuts=(), held_as=jnp.bfloat16):
    result = deviation * jax.random.normal(own_key, extent, jnp.float32)
    if cuts:
        result = result * steps_of(own_key, extent, cuts, -0.22, 0.18)
    return jnp.clip(result, -bound, bound).astype(held_as)


def setup_inputs(seed: int = 0) -> dict:
    splits = jax.random.split(jax.random.key(seed), 11)
    action_old = jnp.clip(jnp.exp(math.log(2.0) - 3.6888794 * jax.random.uniform(splits[0], (FREQ, DIR, NODES), jnp.float32) ** steps_of(splits[0], (FREQ, DIR, NODES), ((0, 4), (2, 64)), -0.2, 0.2)), 0.05, 2.0)
    source = scatter_about(splits[1], (FREQ, DIR, NODES), 0.3, 4.0, ((0, 4), (2, 64)), jnp.float32)
    time_weight = jnp.clip(jnp.exp(math.log(4.0) - 2.0794415 * jax.random.uniform(splits[2], (NODES,), jnp.float32) ** steps_of(splits[2], (NODES,), ((0, 64),), -0.2, 0.2)), 0.5, 4.0)
    group_speed = jnp.clip(jnp.exp(math.log(3.0) - 2.3025851 * jax.random.uniform(splits[3], (FREQ,), jnp.float32) ** steps_of(splits[3], (FREQ,), ((0, 4),), -0.2, 0.2)), 0.3, 3.0)
    normals = scatter_about(splits[4], (2, DEG, NODES), 0.5, 3.0, ((2, 64),), jnp.float32)
    refract = scatter_about(splits[5], (NODES,), 0.6, 4.0, ((0, 64),), jnp.float32)
    freq_shift = scatter_about(splits[6], (NODES,), 0.6, 4.0, ((0, 64),), jnp.float32)
    nbr_list = draw_nbr_list(jax.random.fold_in(splits[10], 71), 0)
    send_nodes = draw_send_nodes(jax.random.fold_in(splits[10], 71), 0)
    adjacency = draw_adjacency(jax.random.fold_in(splits[10], 71), 0)
    return dict(action_old=action_old, source=source, time_weight=time_weight, group_speed=group_speed, normals=normals, refract=refract, freq_shift=freq_shift, nbr_list=nbr_list, send_nodes=send_nodes, adjacency=adjacency)


def reference(action_old, source, time_weight, group_speed, normals, refract, freq_shift, nbr_list, send_nodes, adjacency):
    count = nbr_list.shape[0]
    slots = nbr_list.shape[1]
    width = send_nodes.shape[2]
    local = action_old.shape[2] // count
    angles = 2.0 * math.pi * jnp.arange(DIR).astype(jnp.float32) / DIR
    cosine = jnp.cos(angles)
    sine = jnp.sin(angles)
    valid = nbr_list >= 0
    partner = jnp.where(valid, nbr_list, 0).astype(jnp.int32)
    backward = nbr_list[partner]
    subdomain = jnp.arange(count).astype(jnp.int32)
    slot_ids = jnp.arange(slots).astype(jnp.int32)
    reverse = jnp.sum(jnp.where(backward == subdomain[:, None, None], slot_ids[None, None, :], 0), axis=2).astype(jnp.int32)
    picked = send_nodes[partner, reverse]
    table = (partner[:, :, None] * local + picked).reshape(count, slots * width)
    entries = adjacency.reshape(DEG, count, local)
    position = jnp.clip(entries - local, 0, slots * width - 1)
    remote = jnp.take_along_axis(jnp.broadcast_to(table[None], (DEG, count, slots * width)), position, axis=2)
    global_index = jnp.where(entries < local, subdomain[None, :, None] * local + entries, remote)
    global_index = global_index.reshape(DEG, count * local).astype(jnp.int32)
    own_index = jnp.arange(local).astype(jnp.int32)
    used = (entries != own_index[None, None, :]).reshape(DEG, count * local)

    def flux(k):
        return group_speed[:, None, None] * (cosine[None, :, None] * normals[0, k][None, None, :] + sine[None, :, None] * normals[1, k][None, None, :])

    turning = refract[None, :] * cosine[:, None]
    diagonal = time_weight[None, None, :] + jnp.abs(turning)[None] + jnp.abs(freq_shift)[None, None, :]
    for k in range(DEG):
        diagonal = diagonal + jnp.where(used[k][None, None, :], jnp.maximum(flux(k), 0.0), 0.0)
    steady = time_weight[None, None, :] * action_old + source
    spectra = action_old
    zero_band = jnp.zeros_like(spectra[:1])
    for step in range(ITERS):
        inflow = jnp.maximum(turning, 0.0)[None] * jnp.roll(spectra, 1, axis=1) + jnp.maximum(-turning, 0.0)[None] * jnp.roll(spectra, -1, axis=1)
        lower = jnp.concatenate([zero_band, spectra[:-1]], axis=0)
        upper = jnp.concatenate([spectra[1:], zero_band], axis=0)
        inflow = inflow + jnp.maximum(freq_shift, 0.0)[None, None, :] * lower + jnp.maximum(-freq_shift, 0.0)[None, None, :] * upper
        for k in range(DEG):
            beside = jnp.take(spectra, global_index[k], axis=2)
            inflow = inflow + jnp.where(used[k][None, None, :], jnp.maximum(-flux(k), 0.0), 0.0) * beside
        spectra = (steady + inflow) / diagonal
    return spectra
```

```python
import functools
import math

import jax
import jax.numpy as jnp
import numpy as np
from jax import lax
from jax.experimental import pallas as pl
from jax.experimental.pallas import tpu as pltpu
from jax.sharding import PartitionSpec as P

REACH = 3
ITERS = 3
MESH = pl.DeviceIdType.MESH
F32 = jnp.float32
BF16 = jnp.bfloat16
GROUPS = ((0, 4, 8), (1, 2, 3), (5, 6, 7))
OFFSETS = tuple(sign * reach for reach in range(1, REACH + 1) for sign in (1, -1))


def split(value):
    high = value.astype(BF16)
    low = (value - high.astype(F32)).astype(BF16)
    return high, low


def kernel(
    node_count,
    freq_count,
    old_hbm,
    source_hbm,
    weight_ref,
    refract_ref,
    shift_ref,
    speed_ref,
    normals_ref,
    nbr_ref,
    send_ref,
    adjacency_ref,
    trig_ref,
    out_hbm,
    old_in,
    source_in,
    out_vmem,
    spectra,
    steady,
    inverse,
    edge_weight,
    turn,
    pick_local,
    pick_halo,
    select,
    parts,
    parcel_out,
    parcel_in,
    band_in,
    load_sem,
    store_sem,
    send_sem,
    recv_sem,
    band_send_sem,
    band_recv_sem,
):
    bands, angles, local = old_in.shape
    rows = spectra.shape[2]
    degree = adjacency_ref.shape[0]
    slots, _, width = send_ref.shape
    halo = slots * width
    per_group = len(GROUPS[0])
    half = per_group * rows
    me = lax.axis_index("node")
    band_me = lax.axis_index("freq")

    def node_at(offset):
        return lax.rem(me + offset + node_count, node_count)

    def band_at(offset):
        return lax.rem(band_me + offset + freq_count, freq_count)

    loads = [
        pltpu.make_async_copy(old_hbm, old_in, load_sem.at[0]),
        pltpu.make_async_copy(source_hbm, source_in, load_sem.at[1]),
    ]
    for load in loads:
        load.start()
    barrier = pltpu.get_barrier_semaphore()
    for offset in OFFSETS:
        pl.semaphore_signal(
            barrier, inc=1, device_id={"node": node_at(offset)}, device_id_type=MESH
        )
    for offset in (1, -1):
        pl.semaphore_signal(
            barrier, inc=1, device_id={"freq": band_at(offset)}, device_id_type=MESH
        )

    def parcel(step, group, j):
        piece = pl.ds(j * width, width)
        return pltpu.make_async_remote_copy(
            src_ref=parcel_out.at[step, group, piece],
            dst_ref=parcel_in.at[step, group, piece],
            send_sem=send_sem.at[step, group, j],
            recv_sem=recv_sem.at[step, group, j],
            device_id={"node": node_at(OFFSETS[j])},
            device_id_type=MESH,
        )

    def band_copy(step, side):
        return pltpu.make_async_remote_copy(
            src_ref=spectra.at[step, (bands - 1, 0)[side]],
            dst_ref=band_in.at[step, side],
            send_sem=band_send_sem.at[step, side],
            recv_sem=band_recv_sem.at[step, side],
            device_id={"freq": band_at((1, -1)[side])},
            device_id_type=MESH,
        )

    def send_group(step, group):
        if group == 0:
            for side in range(2):
                band_copy(step, side).start()
        picked = jnp.dot(parts[group], select[...], preferred_element_type=F32)
        picked = picked[:half] + picked[half:]
        picked = jnp.concatenate([picked, jnp.zeros((128 - half, picked.shape[1]), F32)], axis=0)
        parcel_out[step, group] = picked.T[:halo]
        for j in range(len(OFFSETS)):
            parcel(step, group, j).start()

    def set_parts(group, i, value):
        high, low = split(value)
        parts[group, pl.ds(i * rows, rows)] = high
        parts[group, pl.ds(half + i * rows, rows)] = low

    chosen = []
    for offset in OFFSETS:
        target = node_at(offset)
        row = jnp.zeros((1, width), jnp.int32)
        for s in range(slots):
            row = row + jnp.where(nbr_ref[0, s] == target, send_ref[s], 0)
        chosen.append(row)
    fill = jnp.full((1, select.shape[1] - halo), -1, jnp.int32)
    chosen = jnp.concatenate(chosen + [fill], axis=1)
    node_ids = lax.broadcasted_iota(jnp.int32, select.shape, 0)
    select[...] = jnp.where(node_ids == chosen, 1.0, 0.0).astype(BF16)

    loads[0].wait()
    for group, members in enumerate(GROUPS):
        for i, f in enumerate(members):
            value = old_in[f]
            first, last = value[0:1], value[angles - 1 : angles]
            value = jnp.concatenate([value, first, first, last, last], axis=0)
            spectra[0, f] = value
            set_parts(group, i, value)
    pl.semaphore_wait(barrier, len(OFFSETS) + 2)
    for group in range(len(GROUPS)):
        send_group(0, group)

    adjacency = adjacency_ref[...]
    own = lax.broadcasted_iota(jnp.int32, adjacency.shape, 1)
    used = adjacency != own
    relative = adjacency - local
    slot_of = relative // width
    moved = jnp.zeros_like(adjacency)
    for s in range(slots):
        place = jnp.int32(0)
        for j, offset in enumerate(OFFSETS):
            place = place + jnp.where(nbr_ref[0, s] == node_at(-offset), (j - s) * width, 0)
        moved = moved + jnp.where(slot_of == s, place, 0)
    in_halo = jnp.where(adjacency >= local, relative + moved, -1)
    local_ids = lax.broadcasted_iota(jnp.int32, (local, local), 0)
    halo_ids = lax.broadcasted_iota(jnp.int32, (halo, local), 0)
    for k in range(degree):
        pick_local[k] = jnp.where(local_ids == adjacency[k : k + 1], 1.0, 0.0).astype(BF16)
        pick_halo[k] = jnp.where(halo_ids == in_halo[k : k + 1], 1.0, 0.0).astype(BF16)

    cosine = jnp.broadcast_to(trig_ref[:, 0:1], (rows, local))
    sine = jnp.broadcast_to(trig_ref[:, 1:2], (rows, local))
    across = jnp.where(used, normals_ref[0], 0.0)
    along = jnp.where(used, normals_ref[1], 0.0)
    outward = jnp.zeros((rows, local), F32)
    for k in range(degree):
        flux = cosine * across[k : k + 1] + sine * along[k : k + 1]
        outward = outward + jnp.maximum(flux, 0.0)
        edge_weight[k] = jnp.maximum(-flux, 0.0)
    time_weight = weight_ref[...]
    freq_shift = shift_ref[...]
    turning = refract_ref[...] * cosine
    turn[0] = jnp.maximum(turning, 0.0)
    turn[1] = jnp.maximum(-turning, 0.0)
    fixed = time_weight + jnp.abs(turning) + jnp.abs(freq_shift)
    loads[1].wait()
    pad = jnp.zeros((rows - angles, local), F32)
    for f in range(bands):
        inverse[f] = 1.0 / (fixed + speed_ref[0, f] * outward)
        steady[f] = time_weight * spectra[0, f] + jnp.concatenate([source_in[f], pad], axis=0)

    sublane = lax.broadcasted_iota(jnp.int32, (8, local), 0)

    def step_of(step, carry):
        rising = jnp.maximum(freq_shift, 0.0)
        falling = jnp.maximum(-freq_shift, 0.0)
        for group, members in enumerate(GROUPS):
            sums = [jnp.zeros((rows, local), F32) for _ in members]

            def add(sums, left, right_ref):
                for k in range(degree):
                    got = jnp.dot(left, right_ref[k], preferred_element_type=F32)
                    got = got[:half] + got[half:]
                    weight = edge_weight[k]
                    sums = [
                        part + weight * got[i * rows : (i + 1) * rows]
                        for i, part in enumerate(sums)
                    ]
                return sums

            sums = add(sums, parts[group], pick_local)
            for j in range(len(OFFSETS)):
                parcel(step, group, j).wait_recv()
            arrived = parcel_in[step, group].T[:half]
            sums = add(sums, jnp.concatenate(split(arrived), axis=0), pick_halo)
            if group == 0:
                for side in range(2):
                    band_copy(step, side).wait_recv()
            for i, f in enumerate(members):
                value = spectra[step, f]
                inflow = turn[0] * pltpu.roll(value, 1, 0) + turn[1] * pltpu.roll(value, rows - 1, 0)
                if f > 0:
                    below = spectra[step, f - 1]
                else:
                    below = jnp.where(band_me > 0, band_in[step, 0], 0.0)
                if f < bands - 1:
                    above = spectra[step, f + 1]
                else:
                    above = jnp.where(band_me < freq_count - 1, band_in[step, 1], 0.0)
                inflow = inflow + rising * below + falling * above
                value = (steady[f] + inflow + speed_ref[0, f] * sums[i]) * inverse[f]

                @pl.when(step == ITERS - 1)
                def _():
                    out_vmem[f] = value[:angles]
                    pltpu.make_async_copy(out_vmem.at[f], out_hbm.at[f], store_sem.at[f]).start()

                @pl.when(step < ITERS - 1)
                def _():
                    first, last = value[:8], value[rows - 8 :]
                    end = jnp.where(sublane == 7, pltpu.roll(last, 4, 0), last)
                    end = jnp.where(sublane == 4, pltpu.roll(first, 4, 0), end)
                    whole = jnp.concatenate([value[: rows - 8], end], axis=0)
                    spectra[step + 1, f] = whole
                    set_parts(group, i, whole)

            @pl.when(step < ITERS - 1)
            def _():
                send_group(step + 1, group)

        return carry

    lax.fori_loop(0, ITERS, step_of, 0)

    for step in range(ITERS):
        for group in range(len(GROUPS)):
            for j in range(len(OFFSETS)):
                parcel(step, group, j).wait_send()
        for side in range(2):
            band_copy(step, side).wait_send()
    for f in range(bands):
        pltpu.make_async_copy(out_vmem.at[f], out_hbm.at[f], store_sem.at[f]).wait()


def body(
    node_count,
    freq_count,
    action_old,
    source,
    time_weight,
    group_speed,
    normals,
    refract,
    freq_shift,
    nbr_list,
    send_nodes,
    adjacency,
):
    bands, angles, local = action_old.shape
    degree = adjacency.shape[0]
    slots, width = send_nodes.shape[1:]
    rows = -(-(angles + 2) // 8) * 8
    groups = len(GROUPS)
    half = len(GROUPS[0]) * rows
    halo = slots * width
    turns = np.concatenate([np.arange(angles), [0, 0, angles - 1, angles - 1]])
    theta = 2.0 * math.pi * turns / angles
    trig = np.zeros((rows, 128), np.float32)
    trig[:, 0] = np.cos(theta)
    trig[:, 1] = np.sin(theta)
    vmem = pl.BlockSpec(memory_space=pltpu.VMEM)
    smem = pl.BlockSpec(memory_space=pltpu.SMEM)
    anywhere = pl.BlockSpec(memory_space=pl.ANY)
    dma = pltpu.SemaphoreType.DMA
    return pl.pallas_call(
        functools.partial(kernel, node_count, freq_count),
        out_shape=jax.ShapeDtypeStruct(action_old.shape, F32),
        in_specs=[anywhere, anywhere, vmem, vmem, vmem, smem, vmem, smem, vmem, vmem, vmem],
        out_specs=anywhere,
        scratch_shapes=[
            pltpu.VMEM((bands, angles, local), F32),
            pltpu.VMEM((bands, angles, local), F32),
            pltpu.VMEM((bands, angles, local), F32),
            pltpu.VMEM((ITERS, bands, rows, local), F32),
            pltpu.VMEM((bands, rows, local), F32),
            pltpu.VMEM((bands, rows, local), F32),
            pltpu.VMEM((degree, rows, local), F32),
            pltpu.VMEM((2, rows, local), F32),
            pltpu.VMEM((degree, local, local), BF16),
            pltpu.VMEM((degree, halo, local), BF16),
            pltpu.VMEM((local, 256), BF16),
            pltpu.VMEM((groups, 2 * half, local), BF16),
            pltpu.VMEM((ITERS, groups, halo, 128), F32),
            pltpu.VMEM((ITERS, groups, halo, 128), F32),
            pltpu.VMEM((ITERS, 2, rows, local), F32),
            dma((2,)),
            dma((bands,)),
            dma((ITERS, groups, slots)),
            dma((ITERS, groups, slots)),
            dma((ITERS, 2)),
            dma((ITERS, 2)),
        ],
        compiler_params=pltpu.CompilerParams(
            collective_id=0, has_side_effects=True, vmem_limit_bytes=62 * 1024 * 1024
        ),
    )(
        action_old,
        source,
        time_weight[None, :],
        refract[None, :],
        freq_shift[None, :],
        group_speed[None, :],
        normals,
        nbr_list,
        send_nodes.reshape(slots, 1, width),
        adjacency,
        jnp.asarray(trig),
    )


def solution(mesh):
    in_specs = (
        P("freq", None, "node"),
        P("freq", None, "node"),
        P("node"),
        P("freq"),
        P(None, None, "node"),
        P("node"),
        P("node"),
        P("node", None),
        P("node", None, None),
        P(None, "node"),
    )
    return jax.shard_map(
        functools.partial(body, mesh.shape["node"], mesh.shape["freq"]),
        mesh=mesh,
        in_specs=in_specs,
        out_specs=P("freq", None, "node"),
        check_vma=False,
    )
```

```python
import functools
import math

import jax
import jax.numpy as jnp
import numpy as np
from jax import lax
from jax.experimental import pallas as pl
from jax.experimental.pallas import tpu as pltpu
from jax.sharding import PartitionSpec as P

REACH = 3
ITERS = 3
MESH = pl.DeviceIdType.MESH
F32 = jnp.float32
BF16 = jnp.bfloat16
OFFSETS = tuple(sign * reach for reach in range(1, REACH + 1) for sign in (1, -1))
STRIDE = 3
ORDER = (0, 2, 1)
TILE = 256
AHEAD = 4
VMEM_LIMIT = 62 * 1024 * 1024


def split(value):
    high = value.astype(BF16)
    low = (value - high.astype(F32)).astype(BF16)
    return high, low


class Units:
    def __init__(self, jobs):
        self.jobs = jobs
        self.at = [0, 0]
        for unit in range(2):
            self.stage(unit, 0)

    def stage(self, unit, index):
        if index < len(self.jobs[unit]):
            matrix = self.jobs[unit][index][0]()
            pltpu.matmul_push_rhs(matrix, staging_register=index % 2, mxu_index=unit)

    def run(self, count):
        for _ in range(count):
            for unit in range(2):
                index = self.at[unit]
                self.stage(unit, index + 1)
                _, total, high, low = self.jobs[unit][index]
                pltpu.matmul_acc_lhs(total, high(), load_staged_rhs=index % 2)
                pltpu.matmul_acc_lhs(total, low())
                self.at[unit] = index + 1


def kernel(node_count, freq_count, *refs):
    (old_hbm,) = refs[:1]
    speed_ref = refs[5]
    degree = refs[9].shape[0]
    block = refs[14].shape[2]
    count = degree + 1
    specs = [pltpu.ACC(unit)((block, TILE), F32) for unit in range(2) for _ in range(count)]

    def scoped(*totals):
        run(node_count, freq_count, (totals[:count], totals[count:]), *refs)

    pl.run_scoped(scoped, *specs)


def run(
    node_count,
    freq_count,
    totals,
    old_hbm,
    source_hbm,
    weight_ref,
    refract_ref,
    shift_ref,
    speed_ref,
    normals_ref,
    nbr_ref,
    send_ref,
    adjacency_ref,
    trig_ref,
    out_ref,
    old_in,
    source_in,
    spectra,
    base,
    inverse,
    speed_inverse,
    edge_weight,
    turn,
    pick_local,
    pick_halo,
    select,
    parts,
    halo_parts,
    sums,
    parcel_out,
    parcel_in,
    band_in,
    load_sem,
    send_sem,
    recv_sem,
    band_send_sem,
    band_recv_sem,
):
    bands, angles, local = old_in.shape
    groups, block = spectra.shape[1:3]
    edge = band_in.shape[2]
    degree = adjacency_ref.shape[0]
    slots, _, width = send_ref.shape
    halo = slots * width
    members = bands // groups
    me = lax.axis_index("node")
    band_me = lax.axis_index("freq")

    def node_at(offset):
        return lax.rem(me + offset + node_count, node_count)

    def band_at(offset):
        return lax.rem(band_me + offset + freq_count, freq_count)

    loads = [
        pltpu.make_async_copy(old_hbm, old_in, load_sem.at[0]),
        pltpu.make_async_copy(source_hbm, source_in, load_sem.at[1]),
    ]
    for load in loads:
        load.start()
    barrier = pltpu.get_barrier_semaphore()
    for offset in OFFSETS:
        pl.semaphore_signal(
            barrier, inc=1, device_id={"node": node_at(offset)}, device_id_type=MESH
        )
    for offset in (1, -1):
        pl.semaphore_signal(
            barrier, inc=1, device_id={"freq": band_at(offset)}, device_id_type=MESH
        )

    def parcel(step, group, j):
        piece = pl.ds(j * width, width)
        return pltpu.make_async_remote_copy(
            src_ref=parcel_out.at[step, group, piece],
            dst_ref=parcel_in.at[step, group, piece],
            send_sem=send_sem.at[step, group, j],
            recv_sem=recv_sem.at[step, group, j],
            device_id={"node": node_at(OFFSETS[j])},
            device_id_type=MESH,
        )

    def band_copy(step, side):
        row = (block - edge, 0)[side]
        return pltpu.make_async_remote_copy(
            src_ref=spectra.at[step, (groups - 1, 0)[side], pl.ds(row, edge)],
            dst_ref=band_in.at[step, side],
            send_sem=band_send_sem.at[step, side],
            recv_sem=band_recv_sem.at[step, side],
            device_id={"freq": band_at((1, -1)[side])},
            device_id_type=MESH,
        )

    def cut(k):
        return pl.ds(k * TILE, TILE)

    def lhs(group, part, k):
        return lambda: parts[group, part, :, cut(k)]

    def local_jobs(group, entries):
        return [
            [
                (
                    lambda k=k, m=m, unit=unit: pick_local[k, cut(m), cut(unit)],
                    totals[unit][k],
                    lhs(group, 0, m),
                    lhs(group, 1, m),
                )
                for k in entries
                for m in range(local // TILE)
            ]
            for unit in range(2)
        ]

    def halo_jobs(turn_index):
        slot = turn_index % 2
        return [
            [
                (
                    lambda k=k, unit=unit: pick_halo[k, :, cut(unit)],
                    totals[unit][k],
                    lambda: halo_parts[slot, 0],
                    lambda: halo_parts[slot, 1],
                )
                for k in range(degree)
            ]
            for unit in range(2)
        ]

    def select_jobs(group):
        return [
            [
                (
                    lambda unit=unit: select[cut(unit), :],
                    totals[unit][degree],
                    lhs(group, 0, unit),
                    lhs(group, 1, unit),
                )
            ]
            for unit in range(2)
        ]

    def join(*lists):
        return [[job for jobs in lists for job in jobs[unit]] for unit in range(2)]

    def send_group(step, group):
        picked = pltpu.matmul_pop(totals[0][degree]) + pltpu.matmul_pop(totals[1][degree])
        picked = jnp.concatenate([picked, jnp.zeros((128 - block, TILE), F32)], axis=0)
        parcel_out[step, group] = picked.T[:halo]
        for j in range(len(OFFSETS)):
            parcel(step, group, j).start()

    for unit in range(2):
        for total in totals[unit]:
            pltpu.matmul_pop(total)

    chosen = []
    for offset in OFFSETS:
        target = node_at(offset)
        row = jnp.zeros((1, width), jnp.int32)
        for s in range(slots):
            row = row + jnp.where(nbr_ref[0, s] == target, send_ref[s], 0)
        chosen.append(row)
    fill = jnp.full((1, select.shape[1] - halo), -1, jnp.int32)
    chosen = jnp.concatenate(chosen + [fill], axis=1)
    node_ids = lax.broadcasted_iota(jnp.int32, select.shape, 0)
    select[...] = jnp.where(node_ids == chosen, 1.0, 0.0).astype(BF16)

    def pack(ref, group):
        rows = [ref[group + i * STRIDE] for i in range(members)]
        fill = jnp.zeros((block - members * angles, local), F32)
        return jnp.concatenate(rows + [fill], axis=0)

    loads[0].wait()
    for group in ORDER:
        value = pack(old_in, group)
        spectra[0, group] = value
        parts[group, 0], parts[group, 1] = split(value)
    units = Units(join(*[select_jobs(group) for group in ORDER]))
    pl.semaphore_wait(barrier, len(OFFSETS) + 2)
    for side in range(2):
        band_copy(0, side).start()
    for group in ORDER:
        units.run(1)
        send_group(0, group)

    adjacency = adjacency_ref[...]
    own = lax.broadcasted_iota(jnp.int32, adjacency.shape, 1)
    used = adjacency != own
    relative = adjacency - local
    slot_of = relative // width
    moved = jnp.zeros_like(adjacency)
    for s in range(slots):
        place = jnp.int32(0)
        for j, offset in enumerate(OFFSETS):
            place = place + jnp.where(nbr_ref[0, s] == node_at(-offset), (j - s) * width, 0)
        moved = moved + jnp.where(slot_of == s, place, 0)
    in_halo = jnp.where(adjacency >= local, relative + moved, -1)
    chunk = 32
    first_ids = lax.broadcasted_iota(jnp.int32, (chunk, local), 0)

    def fill_from(out, target):
        def fill(c, carry):
            at = pl.multiple_of(c * chunk, chunk)
            ids = first_ids + at
            for k in range(degree):
                hit = jnp.where(ids == target[k : k + 1], 1.0, 0.0)
                out[k, pl.ds(at, chunk), :] = hit.astype(BF16)
            return carry

        lax.fori_loop(0, out.shape[1] // chunk, fill, 0)

    fill_from(pick_local, adjacency)
    fill_from(pick_halo, in_halo)

    period = 2 * angles
    cosine = jnp.broadcast_to(trig_ref[:, 0:1], (period, local))
    sine = jnp.broadcast_to(trig_ref[:, 1:2], (period, local))
    across = jnp.where(used, normals_ref[0], 0.0)
    along = jnp.where(used, normals_ref[1], 0.0)
    outward = jnp.zeros((period, local), F32)
    for k in range(degree):
        flux = cosine * across[k : k + 1] + sine * along[k : k + 1]
        outward = outward + jnp.maximum(flux, 0.0)
        inward = jnp.maximum(-flux, 0.0)
        edge_weight[k, pl.ds(0, period)] = inward
        edge_weight[k, pl.ds(period, block - period)] = inward[: block - period]
    time_weight = weight_ref[...]
    freq_shift = shift_ref[...]
    turning = refract_ref[...] * cosine
    for i, one in enumerate((turning, -turning)):
        one = jnp.maximum(one, 0.0)
        turn[i, pl.ds(0, period)] = one
        turn[i, pl.ds(period, block - period)] = one[: block - period]
    fixed = time_weight + jnp.abs(turning) + jnp.abs(freq_shift)
    outward = jnp.concatenate([outward, outward[: block - period]], axis=0)
    fixed = jnp.concatenate([fixed, fixed[: block - period]], axis=0)
    loads[1].wait()
    row_ids = lax.broadcasted_iota(jnp.int32, (block, local), 0)
    for group in ORDER:
        speed = jnp.full((block, local), speed_ref[0, group], F32)
        for i in range(1, members):
            speed = jnp.where(row_ids >= i * angles, speed_ref[0, group + i * STRIDE], speed)
        one = 1.0 / (fixed + speed * outward)
        inverse[group] = one
        speed_inverse[group] = speed * one
        base[group] = (time_weight * spectra[0, group] + pack(source_in, group)) * one

    rising = jnp.maximum(freq_shift, 0.0)
    falling = jnp.maximum(-freq_shift, 0.0)
    half_rows = lax.broadcasted_iota(jnp.int32, (block, TILE), 0)
    is_first = functools.reduce(jnp.logical_or, [half_rows == i * angles for i in range(members)])
    is_last = functools.reduce(
        jnp.logical_or, [half_rows == i * angles + angles - 1 for i in range(members)]
    )
    tail = jnp.zeros((block - members * angles, TILE), F32)

    def update(step, group, unit):
        columns = cut(unit)
        total = jnp.zeros((block, TILE), F32)
        for k in range(degree):
            total = total + edge_weight[k, :, columns] * pltpu.matmul_pop(totals[unit][k])
        sums[:, columns] = total

    def finish(step, group, unit):
        columns = cut(unit)
        value = spectra[step, group, :, columns]
        before = jnp.where(
            is_first, pltpu.roll(value, block - angles + 1, 0), pltpu.roll(value, 1, 0)
        )
        after = jnp.where(
            is_last, pltpu.roll(value, angles - 1, 0), pltpu.roll(value, block - 1, 0)
        )
        if group > 0:
            below = spectra[step, group - 1, :, columns]
        else:
            rim = band_in[step, 0, :, columns]
            rim = jnp.where(band_me > 0, rim[:angles], 0.0)
            moved = spectra[step, groups - 1, :, columns]
            below = jnp.concatenate([rim, moved[: (members - 1) * angles], tail], axis=0)
        if group < groups - 1:
            above = spectra[step, group + 1, :, columns]
        else:
            rim = band_in[step, 1, :, columns]
            rim = jnp.where(band_me < freq_count - 1, rim[:angles], 0.0)
            moved = spectra[step, 0, :, columns]
            above = jnp.concatenate([moved[angles : members * angles], rim, tail], axis=0)
        inflow = turn[0, :, columns] * before + turn[1, :, columns] * after
        inflow = inflow + rising[:, unit * TILE : (unit + 1) * TILE] * below
        inflow = inflow + falling[:, unit * TILE : (unit + 1) * TILE] * above
        value = base[group, :, columns] + inflow * inverse[group, :, columns]
        value = value + speed_inverse[group, :, columns] * sums[:, columns]
        if step == ITERS - 1:
            for i in range(members):
                out_ref[group + i * STRIDE, :, columns] = value[i * angles : (i + 1) * angles]
        else:
            spectra[step + 1, group, :, columns] = value
            high, low = split(value)
            parts[group, 0, :, columns] = high
            parts[group, 1, :, columns] = low

    turns = [(step, group) for step in range(ITERS) for group in ORDER]
    plan = [local_jobs(turns[0][1], range(AHEAD))]
    for index, (step, group) in enumerate(turns):
        plan.append(local_jobs(group, range(AHEAD, degree)))
        plan.append(halo_jobs(index))
        if index + 1 < len(turns):
            plan.append(local_jobs(turns[index + 1][1], range(AHEAD)))
        if step + 1 < ITERS:
            plan.append(select_jobs(group))
    units = Units(join(*plan))
    per_entry = local // TILE
    units.run(AHEAD * per_entry)
    for index, (step, group) in enumerate(turns):
        for j in range(len(OFFSETS)):
            parcel(step, group, j).wait_recv()
        if group == 0:
            band_copy(step, 0).wait_recv()
        if group == groups - 1:
            band_copy(step, 1).wait_recv()
        arrived = parcel_in[step, group].T[:block]
        arrived = jnp.concatenate([arrived, jnp.zeros((block, TILE - halo), F32)], axis=1)
        halo_parts[index % 2, 0], halo_parts[index % 2, 1] = split(arrived)
        units.run((degree - AHEAD) * per_entry)
        units.run(degree)
        for unit in range(2):
            update(step, group, unit)
        if index + 1 < len(turns):
            units.run(AHEAD * per_entry)
        for unit in range(2):
            finish(step, group, unit)
        if step + 1 < ITERS:
            if group == 0:
                band_copy(step + 1, 1).start()
            if group == groups - 1:
                band_copy(step + 1, 0).start()
            units.run(1)
            send_group(step + 1, group)

    for step in range(ITERS):
        for group in range(groups):
            for j in range(len(OFFSETS)):
                parcel(step, group, j).wait_send()
        for side in range(2):
            band_copy(step, side).wait_send()


def body(
    node_count,
    freq_count,
    action_old,
    source,
    time_weight,
    group_speed,
    normals,
    refract,
    freq_shift,
    nbr_list,
    send_nodes,
    adjacency,
):
    bands, angles, local = action_old.shape
    degree = adjacency.shape[0]
    slots, width = send_nodes.shape[1:]
    groups = STRIDE
    members = bands // groups
    block = -(-members * angles // 16) * 16
    edge = -(-angles // 8) * 8
    halo = slots * width
    theta = 2.0 * math.pi * (np.arange(2 * angles) % angles) / angles
    trig = np.zeros((2 * angles, 128), np.float32)
    trig[:, 0] = np.cos(theta)
    trig[:, 1] = np.sin(theta)
    vmem = pl.BlockSpec(memory_space=pltpu.VMEM)
    smem = pl.BlockSpec(memory_space=pltpu.SMEM)
    anywhere = pl.BlockSpec(memory_space=pl.ANY)
    dma = pltpu.SemaphoreType.DMA
    return pl.pallas_call(
        functools.partial(kernel, node_count, freq_count),
        out_shape=jax.ShapeDtypeStruct(action_old.shape, F32),
        in_specs=[anywhere, anywhere, vmem, vmem, vmem, smem, vmem, smem, vmem, vmem, vmem],
        out_specs=vmem,
        scratch_shapes=[
            pltpu.VMEM((bands, angles, local), F32),
            pltpu.VMEM((bands, angles, local), F32),
            pltpu.VMEM((ITERS, groups, block, local), F32),
            pltpu.VMEM((groups, block, local), F32),
            pltpu.VMEM((groups, block, local), F32),
            pltpu.VMEM((groups, block, local), F32),
            pltpu.VMEM((degree, block, local), F32),
            pltpu.VMEM((2, block, local), F32),
            pltpu.VMEM((degree, local, local), BF16),
            pltpu.VMEM((degree, TILE, local), BF16),
            pltpu.VMEM((local, TILE), BF16),
            pltpu.VMEM((groups, 2, block, local), BF16),
            pltpu.VMEM((2, 2, block, TILE), BF16),
            pltpu.VMEM((block, local), F32),
            pltpu.VMEM((ITERS, groups, halo, 128), F32),
            pltpu.VMEM((ITERS, groups, halo, 128), F32),
            pltpu.VMEM((ITERS, 2, edge, local), F32),
            dma((2,)),
            dma((ITERS, groups, slots)),
            dma((ITERS, groups, slots)),
            dma((ITERS, 2)),
            dma((ITERS, 2)),
        ],
        compiler_params=pltpu.CompilerParams(
            collective_id=0, has_side_effects=True, vmem_limit_bytes=VMEM_LIMIT
        ),
    )(
        action_old,
        source,
        time_weight[None, :],
        refract[None, :],
        freq_shift[None, :],
        group_speed[None, :],
        normals,
        nbr_list,
        send_nodes.reshape(slots, 1, width),
        adjacency,
        jnp.asarray(trig),
    )


def solution(mesh):
    in_specs = (
        P("freq", None, "node"),
        P("freq", None, "node"),
        P("node"),
        P("freq"),
        P(None, None, "node"),
        P("node"),
        P("node"),
        P("node", None),
        P("node", None, None),
        P(None, "node"),
    )
    return jax.shard_map(
        functools.partial(body, mesh.shape["node"], mesh.shape["freq"]),
        mesh=mesh,
        in_specs=in_specs,
        out_specs=P("freq", None, "node"),
        check_vma=False,
    )
```

```python
import functools
import math

import jax
import jax.numpy as jnp
import numpy as np
from jax import lax
from jax.experimental import pallas as pl
from jax.experimental.pallas import tpu as pltpu
from jax.sharding import PartitionSpec as P

REACH = 3
ITERS = 3
MESH = pl.DeviceIdType.MESH
F32 = jnp.float32
BF16 = jnp.bfloat16
OFFSETS = tuple(sign * reach for reach in range(1, REACH + 1) for sign in (1, -1))
STRIDE = 3
ORDER = (0, 2, 1)
TILE = 256
VMEM_LIMIT = 66100000


def split(value):
    high = value.astype(BF16)
    low = (value - high.astype(F32)).astype(BF16)
    return high, low


class Units:
    def __init__(self, jobs):
        self.jobs = jobs
        self.at = [0, 0]
        for unit in range(2):
            self.stage(unit, 0)

    def stage(self, unit, index):
        if index < len(self.jobs[unit]):
            matrix = self.jobs[unit][index][0]()
            pltpu.matmul_push_rhs(matrix, staging_register=index % 2, mxu_index=unit)

    def run(self, count):
        for _ in range(count):
            for unit in range(2):
                index = self.at[unit]
                self.stage(unit, index + 1)
                _, total, high, low = self.jobs[unit][index]
                pltpu.matmul_acc_lhs(total, high(), load_staged_rhs=index % 2)
                pltpu.matmul_acc_lhs(total, low())
                self.at[unit] = index + 1


def kernel(node_count, freq_count, *refs):
    degree = refs[9].shape[0]
    block = refs[14].shape[2]
    count = degree + 1
    specs = [pltpu.ACC(unit)((block, TILE), F32) for unit in range(2) for _ in range(count)]

    def scoped(*totals):
        run(node_count, freq_count, (totals[:count], totals[count:]), *refs)

    pl.run_scoped(scoped, *specs)


def run(
    node_count,
    freq_count,
    totals,
    old_hbm,
    source_hbm,
    weight_hbm,
    refract_hbm,
    shift_hbm,
    speed_hbm,
    normals_hbm,
    nbr_hbm,
    send_hbm,
    adjacency_hbm,
    trig_hbm,
    out_ref,
    old_in,
    source_in,
    spectra,
    base,
    inverse,
    speed_inverse,
    edge_weight,
    turn,
    pick_local,
    pick_halo,
    select,
    parts,
    halo_parts,
    ready,
    parcel_out,
    parcel_in,
    band_in,
    weight_ref,
    refract_ref,
    shift_ref,
    speed_ref,
    normals_ref,
    nbr_ref,
    send_ref,
    adjacency_ref,
    trig_ref,
    load_sem,
    old_sem,
    send_sem,
    recv_sem,
    band_send_sem,
    band_recv_sem,
):
    bands, angles, local = old_in.shape
    groups, block = spectra.shape[1:3]
    edge = band_in.shape[2]
    degree = adjacency_ref.shape[0]
    slots, _, width = send_ref.shape
    halo = slots * width
    members = bands // groups
    me = lax.axis_index("node")
    band_me = lax.axis_index("freq")

    def node_at(offset):
        return lax.rem(me + offset + node_count, node_count)

    def band_at(offset):
        return lax.rem(band_me + offset + freq_count, freq_count)

    def old_load(f):
        return pltpu.make_async_copy(old_hbm.at[f], old_in.at[f], old_sem.at[f])

    pairs = (
        (nbr_hbm, nbr_ref),
        (send_hbm, send_ref),
        (adjacency_hbm, adjacency_ref),
        (normals_hbm, normals_ref),
        (trig_hbm, trig_ref),
        (weight_hbm, weight_ref),
        (refract_hbm, refract_ref),
        (shift_hbm, shift_ref),
        (speed_hbm, speed_ref),
        (source_hbm, source_in),
    )
    loads = [pltpu.make_async_copy(*pair, load_sem.at[i]) for i, pair in enumerate(pairs)]
    for load in loads[:2]:
        load.start()
    for group in ORDER:
        for i in range(members):
            old_load(group + i * STRIDE).start()
    for load in loads[2:]:
        load.start()
    barrier = pltpu.get_barrier_semaphore()
    for offset in OFFSETS:
        pl.semaphore_signal(
            barrier, inc=1, device_id={"node": node_at(offset)}, device_id_type=MESH
        )
    for offset in (1, -1):
        pl.semaphore_signal(
            barrier, inc=1, device_id={"freq": band_at(offset)}, device_id_type=MESH
        )

    def parcel(step, group, j):
        piece = pl.ds(j * width, width)
        return pltpu.make_async_remote_copy(
            src_ref=parcel_out.at[step, group, piece],
            dst_ref=parcel_in.at[step, group, piece],
            send_sem=send_sem.at[step, group, j],
            recv_sem=recv_sem.at[step, group, j],
            device_id={"node": node_at(OFFSETS[j])},
            device_id_type=MESH,
        )

    def band_copy(step, side):
        row = (block - edge, 0)[side]
        return pltpu.make_async_remote_copy(
            src_ref=spectra.at[step, (groups - 1, 0)[side], pl.ds(row, edge)],
            dst_ref=band_in.at[step, side],
            send_sem=band_send_sem.at[step, side],
            recv_sem=band_recv_sem.at[step, side],
            device_id={"freq": band_at((1, -1)[side])},
            device_id_type=MESH,
        )

    def cut(k):
        return pl.ds(k * TILE, TILE)

    def lhs(group, part, k):
        return lambda: parts[group, part, :, cut(k)]

    def local_jobs(group, entries):
        return [
            [
                (
                    lambda k=k, m=m, unit=unit: pick_local[k, cut(m), cut(unit)],
                    totals[unit][k],
                    lhs(group, 0, m),
                    lhs(group, 1, m),
                )
                for k in entries
                for m in range(local // TILE)
            ]
            for unit in range(2)
        ]

    def halo_jobs(turn_index):
        slot = turn_index % 2
        return [
            [
                (
                    lambda k=k, unit=unit: pick_halo[k, :, cut(unit)],
                    totals[unit][k],
                    lambda: halo_parts[slot, 0],
                    lambda: halo_parts[slot, 1],
                )
                for k in range(degree)
            ]
            for unit in range(2)
        ]

    def select_jobs(group):
        return [
            [
                (
                    lambda unit=unit: select[cut(unit), :],
                    totals[unit][degree],
                    lhs(group, 0, unit),
                    lhs(group, 1, unit),
                )
            ]
            for unit in range(2)
        ]

    def join(*lists):
        return [[job for jobs in lists for job in jobs[unit]] for unit in range(2)]

    def send_group(step, group):
        picked = pltpu.matmul_pop(totals[0][degree]) + pltpu.matmul_pop(totals[1][degree])
        picked = jnp.concatenate([picked, jnp.zeros((128 - block, TILE), F32)], axis=0)
        parcel_out[step, group] = picked.T[:halo]
        for j in reversed(range(len(OFFSETS))):
            parcel(step, group, j).start()

    def send_bands(step, group):
        if group == 0:
            band_copy(step, 1).start()
        if group == groups - 1:
            band_copy(step, 0).start()

    for unit in range(2):
        for total in totals[unit]:
            pltpu.matmul_pop(total)

    for load in loads[:2]:
        load.wait()
    chosen = []
    for offset in OFFSETS:
        target = node_at(offset)
        row = jnp.zeros((1, width), jnp.int32)
        for s in range(slots):
            row = row + jnp.where(nbr_ref[0, s] == target, send_ref[s], 0)
        chosen.append(row)
    fill = jnp.full((1, select.shape[1] - halo), -1, jnp.int32)
    chosen = jnp.concatenate(chosen + [fill], axis=1)
    node_ids = lax.broadcasted_iota(jnp.int32, select.shape, 0)
    select[...] = jnp.where(node_ids == chosen, 1.0, 0.0).astype(BF16)

    def pack(ref, group):
        rows = [ref[group + i * STRIDE] for i in range(members)]
        fill = jnp.zeros((block - members * angles, local), F32)
        return jnp.concatenate(rows + [fill], axis=0)

    units = Units(join(*[select_jobs(group) for group in ORDER]))
    pl.semaphore_wait(barrier, len(OFFSETS) + 2)
    for group in ORDER:
        for i in range(members):
            old_load(group + i * STRIDE).wait()
        value = pack(old_in, group)
        spectra[0, group] = value
        parts[group, 0], parts[group, 1] = split(value)
        units.run(1)
        send_group(0, group)
        send_bands(0, group)

    for load in loads[2:-1]:
        load.wait()
    adjacency = adjacency_ref[...]
    own = lax.broadcasted_iota(jnp.int32, adjacency.shape, 1)
    used = adjacency != own
    relative = adjacency - local
    slot_of = relative // width
    moved = jnp.zeros_like(adjacency)
    for s in range(slots):
        place = jnp.int32(0)
        for j, offset in enumerate(OFFSETS):
            place = place + jnp.where(nbr_ref[0, s] == node_at(-offset), (j - s) * width, 0)
        moved = moved + jnp.where(slot_of == s, place, 0)
    in_halo = jnp.where(adjacency >= local, relative + moved, -1)
    chunk = 32
    first_ids = lax.broadcasted_iota(jnp.int32, (chunk, local), 0)

    def fill_from(out, target):
        def fill(c, carry):
            at = pl.multiple_of(c * chunk, chunk)
            ids = first_ids + at
            for k in range(degree):
                hit = jnp.where(ids == target[k : k + 1], 1.0, 0.0)
                out[k, pl.ds(at, chunk), :] = hit.astype(BF16)
            return carry

        lax.fori_loop(0, out.shape[1] // chunk, fill, 0)

    fill_from(pick_local, adjacency)
    fill_from(pick_halo, in_halo)

    period = 2 * angles
    cosine = jnp.broadcast_to(trig_ref[:, 0:1], (period, local))
    sine = jnp.broadcast_to(trig_ref[:, 1:2], (period, local))
    across = jnp.where(used, normals_ref[0], 0.0)
    along = jnp.where(used, normals_ref[1], 0.0)
    outward = jnp.zeros((period, local), F32)
    for k in range(degree):
        flux = cosine * across[k : k + 1] + sine * along[k : k + 1]
        outward = outward + jnp.maximum(flux, 0.0)
        inward = jnp.maximum(-flux, 0.0)
        edge_weight[k, pl.ds(0, period)] = inward
        edge_weight[k, pl.ds(period, block - period)] = inward[: block - period]
    time_weight = weight_ref[...]
    freq_shift = shift_ref[...]
    turning = refract_ref[...] * cosine
    for i, one in enumerate((turning, -turning)):
        one = jnp.maximum(one, 0.0)
        turn[i, pl.ds(0, period)] = one
        turn[i, pl.ds(period, block - period)] = one[: block - period]
    fixed = time_weight + jnp.abs(turning) + jnp.abs(freq_shift)
    outward = jnp.concatenate([outward, outward[: block - period]], axis=0)
    fixed = jnp.concatenate([fixed, fixed[: block - period]], axis=0)
    loads[-1].wait()
    row_ids = lax.broadcasted_iota(jnp.int32, (block, local), 0)
    for group in ORDER:
        speed = jnp.full((block, local), speed_ref[0, group], F32)
        for i in range(1, members):
            speed = jnp.where(row_ids >= i * angles, speed_ref[0, group + i * STRIDE], speed)
        one = 1.0 / (fixed + speed * outward)
        inverse[group] = one
        speed_inverse[group] = speed * one
        base[group] = (time_weight * spectra[0, group] + pack(source_in, group)) * one

    rising = jnp.maximum(freq_shift, 0.0)
    falling = jnp.maximum(-freq_shift, 0.0)
    half_rows = lax.broadcasted_iota(jnp.int32, (block, TILE), 0)
    is_first = functools.reduce(jnp.logical_or, [half_rows == i * angles for i in range(members)])
    is_last = functools.reduce(
        jnp.logical_or, [half_rows == i * angles + angles - 1 for i in range(members)]
    )
    gap = jnp.zeros((angles, TILE), F32)
    tail = jnp.zeros((block - members * angles, TILE), F32)
    edge_rows = lax.broadcasted_iota(jnp.int32, (edge, TILE), 0)

    def gathered(unit):
        total = None
        for k in range(degree):
            term = edge_weight[k, :, cut(unit)] * pltpu.matmul_pop(totals[unit][k])
            total = term if total is None else total + term
        return total

    def prepare(step, group, unit):
        columns = cut(unit)
        value = spectra[step, group, :, columns]
        before = jnp.where(
            is_first, pltpu.roll(value, block - angles + 1, 0), pltpu.roll(value, 1, 0)
        )
        after = jnp.where(
            is_last, pltpu.roll(value, angles - 1, 0), pltpu.roll(value, block - 1, 0)
        )
        if group > 0:
            below = spectra[step, group - 1, :, columns]
        else:
            moved = spectra[step, groups - 1, :, columns]
            below = jnp.concatenate([gap, moved[: (members - 1) * angles], tail], axis=0)
        if group < groups - 1:
            above = spectra[step, group + 1, :, columns]
        else:
            moved = spectra[step, 0, :, columns]
            above = jnp.concatenate([moved[angles : members * angles], gap, tail], axis=0)
        inflow = turn[0, :, columns] * before + turn[1, :, columns] * after
        inflow = inflow + rising[:, unit * TILE : (unit + 1) * TILE] * below
        inflow = inflow + falling[:, unit * TILE : (unit + 1) * TILE] * above
        value = base[group, :, columns] + inflow * inverse[group, :, columns]
        value = value + speed_inverse[group, :, columns] * ready[group, :, columns]
        ready[group, :, columns] = value

    def finish(step, group, unit):
        columns = cut(unit)
        value = ready[group, :, columns]
        value = value + speed_inverse[group, :, columns] * gathered(unit)
        if group == 0:
            rim = band_in[step, 0, :, columns] * rising[:, unit * TILE : (unit + 1) * TILE]
            rim = rim * inverse[group, pl.ds(0, edge), columns]
            rim = jnp.where(jnp.logical_and(edge_rows < angles, band_me > 0), rim, 0.0)
            value = jnp.concatenate([value[:edge] + rim, value[edge:]], axis=0)
        if group == groups - 1:
            rim = band_in[step, 1, :, columns] * falling[:, unit * TILE : (unit + 1) * TILE]
            rim = rim * inverse[group, pl.ds(block - edge, edge), columns]
            rim = jnp.where(
                jnp.logical_and(edge_rows < angles, band_me < freq_count - 1), rim, 0.0
            )
            value = jnp.concatenate(
                [value[: block - edge], value[block - edge :] + rim], axis=0
            )
        if step == ITERS - 1:
            for i in range(members):
                out_ref[group + i * STRIDE, :, columns] = value[i * angles : (i + 1) * angles]
        else:
            spectra[step + 1, group, :, columns] = value
            high, low = split(value)
            parts[group, 0, :, columns] = high
            parts[group, 1, :, columns] = low

    plan = []
    for step in range(ITERS):
        for group in ORDER:
            plan.append(local_jobs(group, range(degree)))
        for index, group in enumerate(ORDER):
            plan.append(halo_jobs(index))
            if step + 1 < ITERS:
                plan.append(select_jobs(group))
    units = Units(join(*plan))
    for step in range(ITERS):
        for group in ORDER:
            units.run(degree * (local // TILE))
            for unit in range(2):
                ready[group, :, cut(unit)] = gathered(unit)
        for group in ORDER:
            for unit in range(2):
                prepare(step, group, unit)
        for index, group in enumerate(ORDER):
            for j in range(len(OFFSETS)):
                parcel(step, group, j).wait_recv()
            arrived = parcel_in[step, group].T[:block]
            arrived = jnp.concatenate([arrived, jnp.zeros((block, TILE - halo), F32)], axis=1)
            halo_parts[index % 2, 0], halo_parts[index % 2, 1] = split(arrived)
            if group == 0:
                band_copy(step, 0).wait_recv()
            if group == groups - 1:
                band_copy(step, 1).wait_recv()
            units.run(degree)
            for unit in range(2):
                finish(step, group, unit)
            if step + 1 < ITERS:
                units.run(1)
                send_group(step + 1, group)
                send_bands(step + 1, group)

    for step in range(ITERS):
        for group in range(groups):
            for j in range(len(OFFSETS)):
                parcel(step, group, j).wait_send()
        for side in range(2):
            band_copy(step, side).wait_send()


def body(
    node_count,
    freq_count,
    action_old,
    source,
    time_weight,
    group_speed,
    normals,
    refract,
    freq_shift,
    nbr_list,
    send_nodes,
    adjacency,
):
    bands, angles, local = action_old.shape
    degree = adjacency.shape[0]
    slots, width = send_nodes.shape[1:]
    groups = STRIDE
    members = bands // groups
    block = -(-members * angles // 16) * 16
    edge = -(-angles // 8) * 8
    halo = slots * width
    theta = 2.0 * math.pi * (np.arange(2 * angles) % angles) / angles
    trig = np.zeros((2 * angles, 128), np.float32)
    trig[:, 0] = np.cos(theta)
    trig[:, 1] = np.sin(theta)
    vmem = pl.BlockSpec(memory_space=pltpu.VMEM)
    anywhere = pl.BlockSpec(memory_space=pl.ANY)
    dma = pltpu.SemaphoreType.DMA
    return pl.pallas_call(
        functools.partial(kernel, node_count, freq_count),
        out_shape=pltpu.VMEM(action_old.shape, F32),
        in_specs=[anywhere] * 11,
        out_specs=vmem,
        scratch_shapes=[
            pltpu.VMEM((bands, angles, local), F32),
            pltpu.VMEM((bands, angles, local), F32),
            pltpu.VMEM((ITERS, groups, block, local), F32),
            pltpu.VMEM((groups, block, local), F32),
            pltpu.VMEM((groups, block, local), F32),
            pltpu.VMEM((groups, block, local), F32),
            pltpu.VMEM((degree, block, local), F32),
            pltpu.VMEM((2, block, local), F32),
            pltpu.VMEM((degree, local, local), BF16),
            pltpu.VMEM((degree, TILE, local), BF16),
            pltpu.VMEM((local, TILE), BF16),
            pltpu.VMEM((groups, 2, block, local), BF16),
            pltpu.VMEM((2, 2, block, TILE), BF16),
            pltpu.VMEM((groups, block, local), F32),
            pltpu.VMEM((ITERS, groups, halo, 128), F32),
            pltpu.VMEM((ITERS, groups, halo, 128), F32),
            pltpu.VMEM((ITERS, 2, edge, local), F32),
            pltpu.VMEM((1, local), F32),
            pltpu.VMEM((1, local), F32),
            pltpu.VMEM((1, local), F32),
            pltpu.SMEM((1, bands), F32),
            pltpu.VMEM((2, degree, local), F32),
            pltpu.SMEM((1, slots), jnp.int32),
            pltpu.VMEM((slots, 1, width), jnp.int32),
            pltpu.VMEM((degree, local), jnp.int32),
            pltpu.VMEM((2 * angles, 128), F32),
            dma((10,)),
            dma((bands,)),
            dma((ITERS, groups, slots)),
            dma((ITERS, groups, slots)),
            dma((ITERS, 2)),
            dma((ITERS, 2)),
        ],
        compiler_params=pltpu.CompilerParams(
            collective_id=0, has_side_effects=True, vmem_limit_bytes=VMEM_LIMIT
        ),
    )(
        action_old,
        source,
        time_weight[None, :],
        refract[None, :],
        freq_shift[None, :],
        group_speed[None, :],
        normals,
        nbr_list,
        send_nodes.reshape(slots, 1, width),
        adjacency,
        jnp.asarray(trig),
    )


def solution(mesh):
    in_specs = (
        P("freq", None, "node"),
        P("freq", None, "node"),
        P("node"),
        P("freq"),
        P(None, None, "node"),
        P("node"),
        P("node"),
        P("node", None),
        P("node", None, None),
        P(None, "node"),
    )
    return jax.shard_map(
        functools.partial(body, mesh.shape["node"], mesh.shape["freq"]),
        mesh=mesh,
        in_specs=in_specs,
        out_specs=P("freq", None, "node"),
        check_vma=False,
    )
```

```python
import functools
import math

import jax
import jax.numpy as jnp
import numpy as np
from jax import lax
from jax.experimental import pallas as pl
from jax.experimental.pallas import tpu as pltpu
from jax.sharding import PartitionSpec as P

REACH = 3
ITERS = 3
MESH = pl.DeviceIdType.MESH
F32 = jnp.float32
BF16 = jnp.bfloat16
OFFSETS = tuple(sign * reach for reach in range(1, REACH + 1) for sign in (1, -1))
STRIDE = 3
ORDER = (0, 2, 1)
TILE = 256
FILL = 4
VMEM_LIMIT = 66100000


def split(value):
    high = value.astype(BF16)
    low = (value - high.astype(F32)).astype(BF16)
    return high, low


class Units:
    def __init__(self, jobs):
        self.jobs = jobs
        self.at = [0, 0]
        for unit in range(2):
            self.stage(unit, 0)

    def stage(self, unit, index):
        if index < len(self.jobs[unit]):
            matrix = self.jobs[unit][index][0]()
            pltpu.matmul_push_rhs(matrix, staging_register=index % 2, mxu_index=unit)

    def run(self, count):
        for _ in range(count):
            for unit in range(2):
                index = self.at[unit]
                self.stage(unit, index + 1)
                _, total, high, low = self.jobs[unit][index]
                pltpu.matmul_acc_lhs(total, high(), load_staged_rhs=index % 2)
                pltpu.matmul_acc_lhs(total, low())
                self.at[unit] = index + 1


def kernel(node_count, freq_count, *refs):
    degree = refs[9].shape[0]
    block = refs[14].shape[2]
    count = degree + 1
    specs = [pltpu.ACC(unit)((block, TILE), F32) for unit in range(2) for _ in range(count)]

    def scoped(*totals):
        run(node_count, freq_count, (totals[:count], totals[count:]), *refs)

    pl.run_scoped(scoped, *specs)


def run(
    node_count,
    freq_count,
    totals,
    old_hbm,
    source_hbm,
    weight_hbm,
    refract_hbm,
    shift_hbm,
    speed_hbm,
    normals_hbm,
    nbr_hbm,
    send_hbm,
    adjacency_hbm,
    trig_hbm,
    out_ref,
    old_in,
    source_in,
    spectra,
    base,
    inverse,
    speed_inverse,
    edge_weight,
    turn,
    pick_local,
    pick_halo,
    select,
    parts,
    halo_parts,
    ready,
    parcel_out,
    parcel_in,
    band_in,
    weight_ref,
    refract_ref,
    shift_ref,
    speed_ref,
    normals_ref,
    nbr_ref,
    send_ref,
    adjacency_ref,
    trig_ref,
    load_sem,
    send_sem,
    recv_sem,
    band_recv_sem,
):
    bands, angles, local = old_in.shape
    groups, block = spectra.shape[1:3]
    edge = band_in.shape[2]
    degree = adjacency_ref.shape[0]
    slots, _, width = send_ref.shape
    halo = slots * width
    members = bands // groups
    me = lax.axis_index("node")
    band_me = lax.axis_index("freq")

    def node_at(offset):
        return lax.rem(me + offset + node_count, node_count)

    def band_at(offset):
        return lax.rem(band_me + offset + freq_count, freq_count)

    pairs = (
        (nbr_hbm, nbr_ref),
        (send_hbm, send_ref),
        (old_hbm, old_in),
        (adjacency_hbm, adjacency_ref),
        (normals_hbm, normals_ref),
        (trig_hbm, trig_ref),
        (weight_hbm, weight_ref),
        (refract_hbm, refract_ref),
        (shift_hbm, shift_ref),
        (speed_hbm, speed_ref),
        (source_hbm, source_in),
    )
    loads = [pltpu.make_async_copy(*pair, load_sem.at[i]) for i, pair in enumerate(pairs)]
    for load in loads:
        load.start()
    barrier = pltpu.get_barrier_semaphore()
    for offset in OFFSETS:
        pl.semaphore_signal(
            barrier, inc=1, device_id={"node": node_at(offset)}, device_id_type=MESH
        )
    for offset in (1, -1):
        pl.semaphore_signal(
            barrier, inc=1, device_id={"freq": band_at(offset)}, device_id_type=MESH
        )

    def parcel(step, group, j):
        piece = pl.ds(j * width, width)
        return pltpu.make_async_remote_copy(
            src_ref=parcel_out.at[step, group, piece],
            dst_ref=parcel_in.at[step, group, piece],
            send_sem=send_sem.at[0],
            recv_sem=recv_sem.at[step, group],
            device_id={"node": node_at(OFFSETS[j])},
            device_id_type=MESH,
        )

    def group_parcels(step, group):
        return pltpu.make_async_remote_copy(
            src_ref=parcel_out.at[step, group],
            dst_ref=parcel_in.at[step, group],
            send_sem=send_sem.at[0],
            recv_sem=recv_sem.at[step, group],
            device_id={"node": node_at(OFFSETS[0])},
            device_id_type=MESH,
        )

    def all_parcels():
        return pltpu.make_async_remote_copy(
            src_ref=parcel_out,
            dst_ref=parcel_in,
            send_sem=send_sem.at[0],
            recv_sem=recv_sem.at[0, 0],
            device_id={"node": node_at(OFFSETS[0])},
            device_id_type=MESH,
        )

    def all_bands():
        return pltpu.make_async_remote_copy(
            src_ref=band_in,
            dst_ref=band_in,
            send_sem=send_sem.at[1],
            recv_sem=band_recv_sem.at[0, 0],
            device_id={"freq": band_at(1)},
            device_id_type=MESH,
        )

    def band_copy(step, side):
        row = (block - edge, 0)[side]
        return pltpu.make_async_remote_copy(
            src_ref=spectra.at[step, (groups - 1, 0)[side], pl.ds(row, edge)],
            dst_ref=band_in.at[step, side],
            send_sem=send_sem.at[1],
            recv_sem=band_recv_sem.at[step, side],
            device_id={"freq": band_at((1, -1)[side])},
            device_id_type=MESH,
        )

    def cut(k):
        return pl.ds(k * TILE, TILE)

    def lhs(group, part, k):
        return lambda: parts[group, part, :, cut(k)]

    def local_jobs(group, entries):
        return [
            [
                (
                    lambda k=k, m=m, unit=unit: pick_local[k, cut(m), cut(unit)],
                    totals[unit][k],
                    lhs(group, 0, m),
                    lhs(group, 1, m),
                )
                for k in entries
                for m in range(local // TILE)
            ]
            for unit in range(2)
        ]

    def halo_jobs(turn_index):
        slot = turn_index % 2
        return [
            [
                (
                    lambda k=k, unit=unit: pick_halo[k, :, cut(unit)],
                    totals[unit][k],
                    lambda: halo_parts[slot, 0],
                    lambda: halo_parts[slot, 1],
                )
                for k in range(degree)
            ]
            for unit in range(2)
        ]

    def select_jobs(group):
        return [
            [
                (
                    lambda unit=unit: select[cut(unit), :],
                    totals[unit][degree],
                    lhs(group, 0, unit),
                    lhs(group, 1, unit),
                )
            ]
            for unit in range(2)
        ]

    def join(*lists):
        return [[job for jobs in lists for job in jobs[unit]] for unit in range(2)]

    def send_group(step, group):
        picked = pltpu.matmul_pop(totals[0][degree]) + pltpu.matmul_pop(totals[1][degree])
        picked = jnp.concatenate([picked, jnp.zeros((128 - block, TILE), F32)], axis=0)
        parcel_out[step, group] = picked.T[:halo]
        for j in reversed(range(len(OFFSETS))):
            parcel(step, group, j).start()

    def send_bands(step, group):
        if group == 0:
            band_copy(step, 1).start()
        if group == groups - 1:
            band_copy(step, 0).start()

    for load in loads[:2]:
        load.wait()
    for unit in range(2):
        for total in totals[unit]:
            pltpu.matmul_pop(total)

    chosen = []
    for offset in OFFSETS:
        target = node_at(offset)
        row = jnp.zeros((1, width), jnp.int32)
        for s in range(slots):
            row = row + jnp.where(nbr_ref[0, s] == target, send_ref[s], 0)
        chosen.append(row)
    fill = jnp.full((1, select.shape[1] - halo), -1, jnp.int32)
    chosen = jnp.concatenate(chosen + [fill], axis=1)
    node_ids = lax.broadcasted_iota(jnp.int32, select.shape, 0)
    select[...] = jnp.where(node_ids == chosen, 1.0, 0.0).astype(BF16)

    def pack(ref, group):
        rows = [ref[group + i * STRIDE] for i in range(members)]
        fill = jnp.zeros((block - members * angles, local), F32)
        return jnp.concatenate(rows + [fill], axis=0)

    for load in loads[3:-1]:
        load.wait()
    adjacency = adjacency_ref[...]
    own = lax.broadcasted_iota(jnp.int32, adjacency.shape, 1)
    used = adjacency != own
    relative = adjacency - local
    slot_of = relative // width
    moved = jnp.zeros_like(adjacency)
    for s in range(slots):
        place = jnp.int32(0)
        for j, offset in enumerate(OFFSETS):
            place = place + jnp.where(nbr_ref[0, s] == node_at(-offset), (j - s) * width, 0)
        moved = moved + jnp.where(slot_of == s, place, 0)
    in_halo = jnp.where(adjacency >= local, relative + moved, -1)
    chunk = 32
    first_ids = lax.broadcasted_iota(jnp.int32, (chunk, local), 0)

    def fill_from(out, target):
        def fill(c, carry):
            at = pl.multiple_of(c * chunk, chunk)
            ids = first_ids + at
            for k in range(degree):
                hit = jnp.where(ids == target[k : k + 1], 1.0, 0.0)
                out[k, pl.ds(at, chunk), :] = hit.astype(BF16)
            return carry

        lax.fori_loop(0, out.shape[1] // chunk, fill, 0)

    fill_from(pick_local, adjacency)
    fill_from(pick_halo, in_halo)

    period = 2 * angles
    cosine = jnp.broadcast_to(trig_ref[:, 0:1], (period, local))
    sine = jnp.broadcast_to(trig_ref[:, 1:2], (period, local))
    across = jnp.where(used, normals_ref[0], 0.0)
    along = jnp.where(used, normals_ref[1], 0.0)
    outward = jnp.zeros((period, local), F32)
    for k in range(degree):
        flux = cosine * across[k : k + 1] + sine * along[k : k + 1]
        outward = outward + jnp.maximum(flux, 0.0)
        inward = jnp.maximum(-flux, 0.0)
        edge_weight[k, pl.ds(0, period)] = inward
        edge_weight[k, pl.ds(period, block - period)] = inward[: block - period]
    time_weight = weight_ref[...]
    freq_shift = shift_ref[...]
    turning = refract_ref[...] * cosine
    for i, one in enumerate((turning, -turning)):
        one = jnp.maximum(one, 0.0)
        turn[i, pl.ds(0, period)] = one
        turn[i, pl.ds(period, block - period)] = one[: block - period]
    fixed = time_weight + jnp.abs(turning) + jnp.abs(freq_shift)
    outward = jnp.concatenate([outward, outward[: block - period]], axis=0)
    fixed = jnp.concatenate([fixed, fixed[: block - period]], axis=0)
    units = Units(join(*[select_jobs(group) for group in ORDER]))
    pl.semaphore_wait(barrier, len(OFFSETS) + 2)
    loads[2].wait()
    for group in ORDER:
        value = pack(old_in, group)
        spectra[0, group] = value
        parts[group, 0], parts[group, 1] = split(value)
        units.run(1)
        send_group(0, group)
        send_bands(0, group)

    loads[-1].wait()
    row_ids = lax.broadcasted_iota(jnp.int32, (block, local), 0)
    for group in ORDER:
        speed = jnp.full((block, local), speed_ref[0, group], F32)
        for i in range(1, members):
            speed = jnp.where(row_ids >= i * angles, speed_ref[0, group + i * STRIDE], speed)
        one = 1.0 / (fixed + speed * outward)
        inverse[group] = one
        speed_inverse[group] = speed * one
        base[group] = (time_weight * spectra[0, group] + pack(source_in, group)) * one

    rising = jnp.maximum(freq_shift, 0.0)
    falling = jnp.maximum(-freq_shift, 0.0)
    half_rows = lax.broadcasted_iota(jnp.int32, (block, TILE), 0)
    is_first = functools.reduce(jnp.logical_or, [half_rows == i * angles for i in range(members)])
    is_last = functools.reduce(
        jnp.logical_or, [half_rows == i * angles + angles - 1 for i in range(members)]
    )
    gap = jnp.zeros((angles, TILE), F32)
    tail = jnp.zeros((block - members * angles, TILE), F32)
    edge_rows = lax.broadcasted_iota(jnp.int32, (edge, TILE), 0)

    def gathered(unit):
        total = None
        for k in range(degree):
            term = edge_weight[k, :, cut(unit)] * pltpu.matmul_pop(totals[unit][k])
            total = term if total is None else total + term
        return total

    def prepare(step, group, unit):
        columns = cut(unit)
        value = spectra[step, group, :, columns]
        before = jnp.where(
            is_first, pltpu.roll(value, block - angles + 1, 0), pltpu.roll(value, 1, 0)
        )
        after = jnp.where(
            is_last, pltpu.roll(value, angles - 1, 0), pltpu.roll(value, block - 1, 0)
        )
        if group > 0:
            below = spectra[step, group - 1, :, columns]
        else:
            moved = spectra[step, groups - 1, :, columns]
            below = jnp.concatenate([gap, moved[: (members - 1) * angles], tail], axis=0)
        if group < groups - 1:
            above = spectra[step, group + 1, :, columns]
        else:
            moved = spectra[step, 0, :, columns]
            above = jnp.concatenate([moved[angles : members * angles], gap, tail], axis=0)
        inflow = turn[0, :, columns] * before + turn[1, :, columns] * after
        inflow = inflow + rising[:, unit * TILE : (unit + 1) * TILE] * below
        inflow = inflow + falling[:, unit * TILE : (unit + 1) * TILE] * above
        ready[group, :, columns] = base[group, :, columns] + inflow * inverse[group, :, columns]

    def finish(step, group, unit):
        columns = cut(unit)
        value = ready[group, :, columns]
        value = value + speed_inverse[group, :, columns] * gathered(unit)
        if group == 0:
            rim = band_in[step, 0, :, columns] * rising[:, unit * TILE : (unit + 1) * TILE]
            rim = rim * inverse[group, pl.ds(0, edge), columns]
            rim = jnp.where(jnp.logical_and(edge_rows < angles, band_me > 0), rim, 0.0)
            value = jnp.concatenate([value[:edge] + rim, value[edge:]], axis=0)
        if group == groups - 1:
            rim = band_in[step, 1, :, columns] * falling[:, unit * TILE : (unit + 1) * TILE]
            rim = rim * inverse[group, pl.ds(block - edge, edge), columns]
            rim = jnp.where(
                jnp.logical_and(edge_rows < angles, band_me < freq_count - 1), rim, 0.0
            )
            value = jnp.concatenate(
                [value[: block - edge], value[block - edge :] + rim], axis=0
            )
        if step == ITERS - 1:
            for i in range(members):
                out_ref[group + i * STRIDE, :, columns] = value[i * angles : (i + 1) * angles]
        else:
            spectra[step + 1, group, :, columns] = value
            high, low = split(value)
            parts[group, 0, :, columns] = high
            parts[group, 1, :, columns] = low

    def arrive(step, index):
        group = ORDER[index]
        group_parcels(step, group).wait_recv()
        arrived = parcel_in[step, group].T[:block]
        arrived = jnp.concatenate([arrived, jnp.zeros((block, TILE - halo), F32)], axis=1)
        halo_parts[index % 2, 0], halo_parts[index % 2, 1] = split(arrived)
        if group == 0:
            band_copy(step, 0).wait_recv()
        if group == groups - 1:
            band_copy(step, 1).wait_recv()

    first = ORDER[0]
    plan = [local_jobs(first, range(FILL))]
    for step in range(ITERS):
        plan.append(local_jobs(first, range(FILL, degree)))
        for group in ORDER[1:]:
            plan.append(local_jobs(group, range(degree)))
        for index, group in enumerate(ORDER):
            plan.append(halo_jobs(index))
            if step + 1 < ITERS:
                if index + 1 == len(ORDER):
                    plan.append(local_jobs(first, range(FILL)))
                plan.append(select_jobs(group))
    units = Units(join(*plan))
    per_entry = local // TILE
    units.run(FILL * per_entry)
    for step in range(ITERS):
        for group in ORDER:
            for unit in range(2):
                prepare(step, group, unit)
        units.run((degree - FILL) * per_entry)
        for group in ORDER:
            if group != first:
                units.run(degree * per_entry)
            for unit in range(2):
                columns = cut(unit)
                local_part = speed_inverse[group, :, columns] * gathered(unit)
                ready[group, :, columns] = ready[group, :, columns] + local_part
        arrive(step, 0)
        for index, group in enumerate(ORDER):
            units.run(degree)
            for unit in range(2):
                finish(step, group, unit)
            if index + 1 < len(ORDER):
                arrive(step, index + 1)
            elif step + 1 < ITERS:
                units.run(FILL * per_entry)
            if step + 1 < ITERS:
                units.run(1)
                send_group(step + 1, group)
                send_bands(step + 1, group)

    all_parcels().wait_send()
    all_bands().wait_send()


def body(
    node_count,
    freq_count,
    action_old,
    source,
    time_weight,
    group_speed,
    normals,
    refract,
    freq_shift,
    nbr_list,
    send_nodes,
    adjacency,
):
    bands, angles, local = action_old.shape
    degree = adjacency.shape[0]
    slots, width = send_nodes.shape[1:]
    groups = STRIDE
    members = bands // groups
    block = -(-members * angles // 16) * 16
    edge = -(-angles // 8) * 8
    halo = slots * width
    theta = 2.0 * math.pi * (np.arange(2 * angles) % angles) / angles
    trig = np.zeros((2 * angles, 128), np.float32)
    trig[:, 0] = np.cos(theta)
    trig[:, 1] = np.sin(theta)
    vmem = pl.BlockSpec(memory_space=pltpu.VMEM)
    anywhere = pl.BlockSpec(memory_space=pl.ANY)
    dma = pltpu.SemaphoreType.DMA
    return pl.pallas_call(
        functools.partial(kernel, node_count, freq_count),
        out_shape=pltpu.VMEM(action_old.shape, F32),
        in_specs=[anywhere] * 11,
        out_specs=vmem,
        scratch_shapes=[
            pltpu.VMEM((bands, angles, local), F32),
            pltpu.VMEM((bands, angles, local), F32),
            pltpu.VMEM((ITERS, groups, block, local), F32),
            pltpu.VMEM((groups, block, local), F32),
            pltpu.VMEM((groups, block, local), F32),
            pltpu.VMEM((groups, block, local), F32),
            pltpu.VMEM((degree, block, local), F32),
            pltpu.VMEM((2, block, local), F32),
            pltpu.VMEM((degree, local, local), BF16),
            pltpu.VMEM((degree, TILE, local), BF16),
            pltpu.VMEM((local, TILE), BF16),
            pltpu.VMEM((groups, 2, block, local), BF16),
            pltpu.VMEM((2, 2, block, TILE), BF16),
            pltpu.VMEM((groups, block, local), F32),
            pltpu.VMEM((ITERS, groups, halo, 128), F32),
            pltpu.VMEM((ITERS, groups, halo, 128), F32),
            pltpu.VMEM((ITERS, 2, edge, local), F32),
            pltpu.VMEM((1, local), F32),
            pltpu.VMEM((1, local), F32),
            pltpu.VMEM((1, local), F32),
            pltpu.SMEM((1, bands), F32),
            pltpu.VMEM((2, degree, local), F32),
            pltpu.SMEM((1, slots), jnp.int32),
            pltpu.VMEM((slots, 1, width), jnp.int32),
            pltpu.VMEM((degree, local), jnp.int32),
            pltpu.VMEM((2 * angles, 128), F32),
            dma((11,)),
            dma((2,)),
            dma((ITERS, groups)),
            dma((ITERS, 2)),
        ],
        compiler_params=pltpu.CompilerParams(
            collective_id=0, has_side_effects=True, vmem_limit_bytes=VMEM_LIMIT
        ),
    )(
        action_old,
        source,
        time_weight[None, :],
        refract[None, :],
        freq_shift[None, :],
        group_speed[None, :],
        normals,
        nbr_list,
        send_nodes.reshape(slots, 1, width),
        adjacency,
        jnp.asarray(trig),
    )


def solution(mesh):
    in_specs = (
        P("freq", None, "node"),
        P("freq", None, "node"),
        P("node"),
        P("freq"),
        P(None, None, "node"),
        P("node"),
        P("node"),
        P("node", None),
        P("node", None, None),
        P(None, "node"),
    )
    return jax.shard_map(
        functools.partial(body, mesh.shape["node"], mesh.shape["freq"]),
        mesh=mesh,
        in_specs=in_specs,
        out_specs=P("freq", None, "node"),
        check_vma=False,
    )
```

```python
import functools
import math

import jax
import jax.numpy as jnp
import numpy as np
from jax import lax
from jax.experimental import pallas as pl
from jax.experimental.pallas import tpu as pltpu
from jax.sharding import PartitionSpec as P

REACH = 3
ITERS = 3
MESH = pl.DeviceIdType.MESH
F32 = jnp.float32
BF16 = jnp.bfloat16
OFFSETS = tuple(sign * reach for reach in range(1, REACH + 1) for sign in (1, -1))
STRIDE = 3
ORDER = (0, 2, 1)
TILE = 256
FILL = 4
VMEM_LIMIT = 66100000


def split(value):
    high = value.astype(BF16)
    low = (value - high.astype(F32)).astype(BF16)
    return high, low


class Units:
    def __init__(self, jobs):
        self.jobs = jobs
        self.at = [0, 0]
        for unit in range(2):
            self.stage(unit, 0)

    def stage(self, unit, index):
        if index < len(self.jobs[unit]):
            matrix = self.jobs[unit][index][0]()
            pltpu.matmul_push_rhs(matrix, staging_register=index % 2, mxu_index=unit)

    def run(self, count):
        for _ in range(count):
            for unit in range(2):
                index = self.at[unit]
                self.stage(unit, index + 1)
                _, total, high, low = self.jobs[unit][index]
                pltpu.matmul_acc_lhs(total, high(), load_staged_rhs=index % 2)
                pltpu.matmul_acc_lhs(total, low())
                self.at[unit] = index + 1


def kernel(node_count, freq_count, *refs):
    degree = refs[9].shape[0]
    block = refs[14].shape[2]
    count = degree + 1
    specs = [pltpu.ACC(unit)((block, TILE), F32) for unit in range(2) for _ in range(count)]

    def scoped(*totals):
        run(node_count, freq_count, (totals[:count], totals[count:]), *refs)

    pl.run_scoped(scoped, *specs)


def run(
    node_count,
    freq_count,
    totals,
    old_hbm,
    source_hbm,
    weight_hbm,
    refract_hbm,
    shift_hbm,
    speed_hbm,
    normals_hbm,
    nbr_hbm,
    send_hbm,
    adjacency_hbm,
    trig_hbm,
    out_ref,
    old_in,
    source_in,
    spectra,
    base,
    inverse,
    speed_inverse,
    edge_weight,
    turn,
    pick_local,
    pick_halo,
    select,
    parts,
    halo_parts,
    ready,
    parcel_out,
    parcel_in,
    band_in,
    weight_ref,
    refract_ref,
    shift_ref,
    speed_ref,
    normals_ref,
    nbr_ref,
    send_ref,
    adjacency_ref,
    trig_ref,
    load_sem,
    send_sem,
    recv_sem,
    band_recv_sem,
):
    bands, angles, local = old_in.shape
    groups, block = spectra.shape[1:3]
    edge = band_in.shape[2]
    degree = adjacency_ref.shape[0]
    slots, _, width = send_ref.shape
    halo = slots * width
    members = bands // groups
    me = lax.axis_index("node")
    band_me = lax.axis_index("freq")

    def node_at(offset):
        return lax.rem(me + offset + node_count, node_count)

    def band_at(offset):
        return lax.rem(band_me + offset + freq_count, freq_count)

    pairs = (
        (nbr_hbm, nbr_ref),
        (send_hbm, send_ref),
        (old_hbm, old_in),
        (adjacency_hbm, adjacency_ref),
        (normals_hbm, normals_ref),
        (trig_hbm, trig_ref),
        (weight_hbm, weight_ref),
        (refract_hbm, refract_ref),
        (shift_hbm, shift_ref),
        (speed_hbm, speed_ref),
        (source_hbm, source_in),
    )
    loads = [pltpu.make_async_copy(*pair, load_sem.at[i]) for i, pair in enumerate(pairs)]
    for load in loads:
        load.start()
    barrier = pltpu.get_barrier_semaphore()
    for offset in OFFSETS:
        pl.semaphore_signal(
            barrier, inc=1, device_id={"node": node_at(offset)}, device_id_type=MESH
        )
    for offset in (1, -1):
        pl.semaphore_signal(
            barrier, inc=1, device_id={"freq": band_at(offset)}, device_id_type=MESH
        )

    def parcel(step, group, j):
        piece = pl.ds(j * width, width)
        return pltpu.make_async_remote_copy(
            src_ref=parcel_out.at[step, group, piece],
            dst_ref=parcel_in.at[step, group, piece],
            send_sem=send_sem.at[0],
            recv_sem=recv_sem.at[step, group],
            device_id={"node": node_at(OFFSETS[j])},
            device_id_type=MESH,
        )

    def group_parcels(step, group):
        return pltpu.make_async_remote_copy(
            src_ref=parcel_out.at[step, group],
            dst_ref=parcel_in.at[step, group],
            send_sem=send_sem.at[0],
            recv_sem=recv_sem.at[step, group],
            device_id={"node": node_at(OFFSETS[0])},
            device_id_type=MESH,
        )

    def all_parcels():
        return pltpu.make_async_remote_copy(
            src_ref=parcel_out,
            dst_ref=parcel_in,
            send_sem=send_sem.at[0],
            recv_sem=recv_sem.at[0, 0],
            device_id={"node": node_at(OFFSETS[0])},
            device_id_type=MESH,
        )

    def all_bands():
        return pltpu.make_async_remote_copy(
            src_ref=band_in,
            dst_ref=band_in,
            send_sem=send_sem.at[1],
            recv_sem=band_recv_sem.at[0, 0],
            device_id={"freq": band_at(1)},
            device_id_type=MESH,
        )

    def band_copy(step, side):
        row = (block - edge, 0)[side]
        return pltpu.make_async_remote_copy(
            src_ref=spectra.at[step, (groups - 1, 0)[side], pl.ds(row, edge)],
            dst_ref=band_in.at[step, side],
            send_sem=send_sem.at[1],
            recv_sem=band_recv_sem.at[step, side],
            device_id={"freq": band_at((1, -1)[side])},
            device_id_type=MESH,
        )

    def cut(k):
        return pl.ds(k * TILE, TILE)

    def lhs(group, part, k):
        return lambda: parts[group, part, :, cut(k)]

    def local_jobs(group, entries):
        return [
            [
                (
                    lambda k=k, m=m, unit=unit: pick_local[k, cut(m), cut(unit)],
                    totals[unit][k],
                    lhs(group, 0, m),
                    lhs(group, 1, m),
                )
                for k in entries
                for m in range(local // TILE)
            ]
            for unit in range(2)
        ]

    def halo_jobs(turn_index):
        slot = turn_index % 2
        return [
            [
                (
                    lambda k=k, unit=unit: pick_halo[k, :, cut(unit)],
                    totals[unit][k],
                    lambda: halo_parts[slot, 0],
                    lambda: halo_parts[slot, 1],
                )
                for k in range(degree)
            ]
            for unit in range(2)
        ]

    def select_jobs(group):
        return [
            [
                (
                    lambda unit=unit: select[cut(unit), :],
                    totals[unit][degree],
                    lhs(group, 0, unit),
                    lhs(group, 1, unit),
                )
            ]
            for unit in range(2)
        ]

    def join(*lists):
        return [[job for jobs in lists for job in jobs[unit]] for unit in range(2)]

    def send_group(step, group):
        picked = pltpu.matmul_pop(totals[0][degree]) + pltpu.matmul_pop(totals[1][degree])
        picked = jnp.concatenate([picked, jnp.zeros((128 - block, TILE), F32)], axis=0)
        parcel_out[step, group] = picked.T[:halo]
        for j in reversed(range(len(OFFSETS))):
            parcel(step, group, j).start()

    def send_bands(step, group):
        if group == 0:
            band_copy(step, 1).start()
        if group == groups - 1:
            band_copy(step, 0).start()

    for load in loads[:2]:
        load.wait()
    for unit in range(2):
        for total in totals[unit]:
            pltpu.matmul_pop(total)

    chosen = []
    for offset in OFFSETS:
        target = node_at(offset)
        row = jnp.zeros((1, width), jnp.int32)
        for s in range(slots):
            row = row + jnp.where(nbr_ref[0, s] == target, send_ref[s], 0)
        chosen.append(row)
    fill = jnp.full((1, select.shape[1] - halo), -1, jnp.int32)
    chosen = jnp.concatenate(chosen + [fill], axis=1)
    node_ids = lax.broadcasted_iota(jnp.int32, select.shape, 0)
    select[...] = jnp.where(node_ids == chosen, 1.0, 0.0).astype(BF16)

    def pack(ref, group):
        rows = [ref[group + i * STRIDE] for i in range(members)]
        fill = jnp.zeros((block - members * angles, local), F32)
        return jnp.concatenate(rows + [fill], axis=0)

    for load in loads[3:-1]:
        load.wait()
    adjacency = adjacency_ref[...]
    own = lax.broadcasted_iota(jnp.int32, adjacency.shape, 1)
    used = adjacency != own
    relative = adjacency - local
    slot_of = relative // width
    moved = jnp.zeros_like(adjacency)
    for s in range(slots):
        place = jnp.int32(0)
        for j, offset in enumerate(OFFSETS):
            place = place + jnp.where(nbr_ref[0, s] == node_at(-offset), (j - s) * width, 0)
        moved = moved + jnp.where(slot_of == s, place, 0)
    in_halo = jnp.where(adjacency >= local, relative + moved, -1)
    chunk = 32
    first_ids = lax.broadcasted_iota(jnp.int32, (chunk, local), 0)

    def fill_from(out, target):
        def fill(c, carry):
            at = pl.multiple_of(c * chunk, chunk)
            ids = first_ids + at
            for k in range(degree):
                hit = jnp.where(ids == target[k : k + 1], 1.0, 0.0)
                out[k, pl.ds(at, chunk), :] = hit.astype(BF16)
            return carry

        lax.fori_loop(0, out.shape[1] // chunk, fill, 0)

    fill_from(pick_local, adjacency)
    units = Units(join(*[select_jobs(group) for group in ORDER]))
    pl.semaphore_wait(barrier, len(OFFSETS) + 2)
    loads[2].wait()
    for group in ORDER:
        value = pack(old_in, group)
        spectra[0, group] = value
        parts[group, 0], parts[group, 1] = split(value)
        send_bands(0, group)
        units.run(1)
        send_group(0, group)

    fill_from(pick_halo, in_halo)

    period = 2 * angles
    cosine = jnp.broadcast_to(trig_ref[:, 0:1], (period, local))
    sine = jnp.broadcast_to(trig_ref[:, 1:2], (period, local))
    across = jnp.where(used, normals_ref[0], 0.0)
    along = jnp.where(used, normals_ref[1], 0.0)
    outward = jnp.zeros((period, local), F32)
    for k in range(degree):
        flux = cosine * across[k : k + 1] + sine * along[k : k + 1]
        outward = outward + jnp.maximum(flux, 0.0)
        inward = jnp.maximum(-flux, 0.0)
        edge_weight[k, pl.ds(0, period)] = inward
        edge_weight[k, pl.ds(period, block - period)] = inward[: block - period]
    time_weight = weight_ref[...]
    freq_shift = shift_ref[...]
    turning = refract_ref[...] * cosine
    for i, one in enumerate((turning, -turning)):
        one = jnp.maximum(one, 0.0)
        turn[i, pl.ds(0, period)] = one
        turn[i, pl.ds(period, block - period)] = one[: block - period]
    fixed = time_weight + jnp.abs(turning) + jnp.abs(freq_shift)
    outward = jnp.concatenate([outward, outward[: block - period]], axis=0)
    fixed = jnp.concatenate([fixed, fixed[: block - period]], axis=0)
    loads[-1].wait()
    row_ids = lax.broadcasted_iota(jnp.int32, (block, local), 0)
    for group in ORDER:
        speed = jnp.full((block, local), speed_ref[0, group], F32)
        for i in range(1, members):
            speed = jnp.where(row_ids >= i * angles, speed_ref[0, group + i * STRIDE], speed)
        one = 1.0 / (fixed + speed * outward)
        inverse[group] = one
        speed_inverse[group] = speed * one
        base[group] = (time_weight * spectra[0, group] + pack(source_in, group)) * one

    rising = jnp.maximum(freq_shift, 0.0)
    falling = jnp.maximum(-freq_shift, 0.0)
    half_rows = lax.broadcasted_iota(jnp.int32, (block, TILE), 0)
    is_first = functools.reduce(jnp.logical_or, [half_rows == i * angles for i in range(members)])
    is_last = functools.reduce(
        jnp.logical_or, [half_rows == i * angles + angles - 1 for i in range(members)]
    )
    gap = jnp.zeros((angles, TILE), F32)
    tail = jnp.zeros((block - members * angles, TILE), F32)
    edge_rows = lax.broadcasted_iota(jnp.int32, (edge, TILE), 0)

    def gathered(unit):
        total = None
        for k in range(degree):
            term = edge_weight[k, :, cut(unit)] * pltpu.matmul_pop(totals[unit][k])
            total = term if total is None else total + term
        return total

    def prepare(step, group, unit):
        columns = cut(unit)
        value = spectra[step, group, :, columns]
        before = jnp.where(
            is_first, pltpu.roll(value, block - angles + 1, 0), pltpu.roll(value, 1, 0)
        )
        after = jnp.where(
            is_last, pltpu.roll(value, angles - 1, 0), pltpu.roll(value, block - 1, 0)
        )
        if group > 0:
            below = spectra[step, group - 1, :, columns]
        else:
            moved = spectra[step, groups - 1, :, columns]
            below = jnp.concatenate([gap, moved[: (members - 1) * angles], tail], axis=0)
        if group < groups - 1:
            above = spectra[step, group + 1, :, columns]
        else:
            moved = spectra[step, 0, :, columns]
            above = jnp.concatenate([moved[angles : members * angles], gap, tail], axis=0)
        inflow = turn[0, :, columns] * before + turn[1, :, columns] * after
        inflow = inflow + rising[:, unit * TILE : (unit + 1) * TILE] * below
        inflow = inflow + falling[:, unit * TILE : (unit + 1) * TILE] * above
        ready[group, :, columns] = base[group, :, columns] + inflow * inverse[group, :, columns]

    def finish(step, group, unit):
        columns = cut(unit)
        value = ready[group, :, columns]
        value = value + speed_inverse[group, :, columns] * gathered(unit)
        if group == 0:
            rim = band_in[step, 0, :, columns] * rising[:, unit * TILE : (unit + 1) * TILE]
            rim = rim * inverse[group, pl.ds(0, edge), columns]
            rim = jnp.where(jnp.logical_and(edge_rows < angles, band_me > 0), rim, 0.0)
            value = jnp.concatenate([value[:edge] + rim, value[edge:]], axis=0)
        if group == groups - 1:
            rim = band_in[step, 1, :, columns] * falling[:, unit * TILE : (unit + 1) * TILE]
            rim = rim * inverse[group, pl.ds(block - edge, edge), columns]
            rim = jnp.where(
                jnp.logical_and(edge_rows < angles, band_me < freq_count - 1), rim, 0.0
            )
            value = jnp.concatenate(
                [value[: block - edge], value[block - edge :] + rim], axis=0
            )
        if step == ITERS - 1:
            for i in range(members):
                out_ref[group + i * STRIDE, :, columns] = value[i * angles : (i + 1) * angles]
        else:
            spectra[step + 1, group, :, columns] = value
            high, low = split(value)
            parts[group, 0, :, columns] = high
            parts[group, 1, :, columns] = low

    def arrive(step, index):
        group = ORDER[index]
        group_parcels(step, group).wait_recv()
        arrived = parcel_in[step, group].T[:block]
        arrived = jnp.concatenate([arrived, jnp.zeros((block, TILE - halo), F32)], axis=1)
        halo_parts[index % 2, 0], halo_parts[index % 2, 1] = split(arrived)

    def arrive_band(step, group):
        if group == 0:
            band_copy(step, 0).wait_recv()
        if group == groups - 1:
            band_copy(step, 1).wait_recv()

    first = ORDER[0]
    plan = [local_jobs(first, range(FILL))]
    for step in range(ITERS):
        plan.append(local_jobs(first, range(FILL, degree)))
        for group in ORDER[1:]:
            plan.append(local_jobs(group, range(degree)))
        for index, group in enumerate(ORDER):
            plan.append(halo_jobs(index))
            if step + 1 < ITERS:
                if index + 1 == len(ORDER):
                    plan.append(local_jobs(first, range(FILL)))
                plan.append(select_jobs(group))
    units = Units(join(*plan))
    per_entry = local // TILE
    units.run(FILL * per_entry)
    for step in range(ITERS):
        for group in ORDER:
            for unit in range(2):
                prepare(step, group, unit)
        units.run((degree - FILL) * per_entry)
        for group in ORDER:
            if group != first:
                units.run(degree * per_entry)
            for unit in range(2):
                columns = cut(unit)
                local_part = speed_inverse[group, :, columns] * gathered(unit)
                ready[group, :, columns] = ready[group, :, columns] + local_part
        arrive(step, 0)
        for index, group in enumerate(ORDER):
            units.run(degree)
            arrive_band(step, group)
            for unit in range(2):
                finish(step, group, unit)
            if step + 1 < ITERS:
                send_bands(step + 1, group)
            if index + 1 < len(ORDER):
                arrive(step, index + 1)
            elif step + 1 < ITERS:
                units.run(FILL * per_entry)
            if step + 1 < ITERS:
                units.run(1)
                send_group(step + 1, group)

    all_parcels().wait_send()
    all_bands().wait_send()


def body(
    node_count,
    freq_count,
    action_old,
    source,
    time_weight,
    group_speed,
    normals,
    refract,
    freq_shift,
    nbr_list,
    send_nodes,
    adjacency,
):
    bands, angles, local = action_old.shape
    degree = adjacency.shape[0]
    slots, width = send_nodes.shape[1:]
    groups = STRIDE
    members = bands // groups
    block = -(-members * angles // 16) * 16
    edge = -(-angles // 8) * 8
    halo = slots * width
    theta = 2.0 * math.pi * (np.arange(2 * angles) % angles) / angles
    trig = np.zeros((2 * angles, 128), np.float32)
    trig[:, 0] = np.cos(theta)
    trig[:, 1] = np.sin(theta)
    vmem = pl.BlockSpec(memory_space=pltpu.VMEM)
    anywhere = pl.BlockSpec(memory_space=pl.ANY)
    dma = pltpu.SemaphoreType.DMA
    return pl.pallas_call(
        functools.partial(kernel, node_count, freq_count),
        out_shape=pltpu.VMEM(action_old.shape, F32),
        in_specs=[anywhere] * 11,
        out_specs=vmem,
        scratch_shapes=[
            pltpu.VMEM((bands, angles, local), F32),
            pltpu.VMEM((bands, angles, local), F32),
            pltpu.VMEM((ITERS, groups, block, local), F32),
            pltpu.VMEM((groups, block, local), F32),
            pltpu.VMEM((groups, block, local), F32),
            pltpu.VMEM((groups, block, local), F32),
            pltpu.VMEM((degree, block, local), F32),
            pltpu.VMEM((2, block, local), F32),
            pltpu.VMEM((degree, local, local), BF16),
            pltpu.VMEM((degree, TILE, local), BF16),
            pltpu.VMEM((local, TILE), BF16),
            pltpu.VMEM((groups, 2, block, local), BF16),
            pltpu.VMEM((2, 2, block, TILE), BF16),
            pltpu.VMEM((groups, block, local), F32),
            pltpu.VMEM((ITERS, groups, halo, 128), F32),
            pltpu.VMEM((ITERS, groups, halo, 128), F32),
            pltpu.VMEM((ITERS, 2, edge, local), F32),
            pltpu.VMEM((1, local), F32),
            pltpu.VMEM((1, local), F32),
            pltpu.VMEM((1, local), F32),
            pltpu.SMEM((1, bands), F32),
            pltpu.VMEM((2, degree, local), F32),
            pltpu.SMEM((1, slots), jnp.int32),
            pltpu.VMEM((slots, 1, width), jnp.int32),
            pltpu.VMEM((degree, local), jnp.int32),
            pltpu.VMEM((2 * angles, 128), F32),
            dma((11,)),
            dma((2,)),
            dma((ITERS, groups)),
            dma((ITERS, 2)),
        ],
        compiler_params=pltpu.CompilerParams(
            collective_id=0, has_side_effects=True, vmem_limit_bytes=VMEM_LIMIT
        ),
    )(
        action_old,
        source,
        time_weight[None, :],
        refract[None, :],
        freq_shift[None, :],
        group_speed[None, :],
        normals,
        nbr_list,
        send_nodes.reshape(slots, 1, width),
        adjacency,
        jnp.asarray(trig),
    )


def solution(mesh):
    in_specs = (
        P("freq", None, "node"),
        P("freq", None, "node"),
        P("node"),
        P("freq"),
        P(None, None, "node"),
        P("node"),
        P("node"),
        P("node", None),
        P("node", None, None),
        P(None, "node"),
    )
    return jax.shard_map(
        functools.partial(body, mesh.shape["node"], mesh.shape["freq"]),
        mesh=mesh,
        in_specs=in_specs,
        out_specs=P("freq", None, "node"),
        check_vma=False,
    )
```

```python
import functools
import math

import jax
import jax.numpy as jnp
import numpy as np
from jax import lax
from jax.experimental import pallas as pl
from jax.experimental.pallas import tpu as pltpu
from jax.sharding import PartitionSpec as P

REACH = 3
ITERS = 3
MESH = pl.DeviceIdType.MESH
F32 = jnp.float32
BF16 = jnp.bfloat16
OFFSETS = tuple(sign * reach for reach in range(1, REACH + 1) for sign in (1, -1))
STRIDE = 3
ORDER = (0, 2, 1)
TILE = 256
FILL = 4
VMEM_LIMIT = 66100000


def split(value):
    high = value.astype(BF16)
    low = (value - high.astype(F32)).astype(BF16)
    return high, low


class Units:
    def __init__(self, jobs):
        self.jobs = jobs
        self.at = [0, 0]
        for unit in range(2):
            self.stage(unit, 0)

    def stage(self, unit, index):
        if index < len(self.jobs[unit]):
            matrix = self.jobs[unit][index][0]()
            pltpu.matmul_push_rhs(matrix, staging_register=index % 2, mxu_index=unit)

    def run(self, count):
        for _ in range(count):
            for unit in range(2):
                index = self.at[unit]
                self.stage(unit, index + 1)
                _, total, high, low = self.jobs[unit][index]
                pltpu.matmul_acc_lhs(total, high(), load_staged_rhs=index % 2)
                pltpu.matmul_acc_lhs(total, low())
                self.at[unit] = index + 1


def kernel(node_count, freq_count, *refs):
    degree = refs[9].shape[0]
    block = refs[14].shape[2]
    count = degree + 1
    specs = [pltpu.ACC(unit)((block, TILE), F32) for unit in range(2) for _ in range(count)]

    def scoped(*totals):
        run(node_count, freq_count, (totals[:count], totals[count:]), *refs)

    pl.run_scoped(scoped, *specs)


def run(
    node_count,
    freq_count,
    totals,
    old_hbm,
    source_hbm,
    weight_hbm,
    refract_hbm,
    shift_hbm,
    speed_hbm,
    normals_hbm,
    nbr_hbm,
    send_hbm,
    adjacency_hbm,
    trig_hbm,
    out_ref,
    old_in,
    source_in,
    spectra,
    base,
    inverse,
    speed_inverse,
    edge_weight,
    turn,
    pick_local,
    pick_halo,
    select,
    parts,
    halo_parts,
    ready,
    parcel_out,
    parcel_in,
    band_in,
    weight_ref,
    refract_ref,
    shift_ref,
    speed_ref,
    normals_ref,
    nbr_ref,
    send_ref,
    adjacency_ref,
    trig_ref,
    load_sem,
    send_sem,
    recv_sem,
    band_recv_sem,
):
    bands, angles, local = old_in.shape
    groups, block = spectra.shape[1:3]
    edge = band_in.shape[2]
    degree = adjacency_ref.shape[0]
    slots, _, width = send_ref.shape
    halo = slots * width
    members = bands // groups
    me = lax.axis_index("node")
    band_me = lax.axis_index("freq")

    def node_at(offset):
        return lax.rem(me + offset + node_count, node_count)

    def band_at(offset):
        return lax.rem(band_me + offset + freq_count, freq_count)

    pairs = (
        (nbr_hbm, nbr_ref),
        (send_hbm, send_ref),
        (old_hbm, old_in),
        (adjacency_hbm, adjacency_ref),
        (normals_hbm, normals_ref),
        (trig_hbm, trig_ref),
        (weight_hbm, weight_ref),
        (refract_hbm, refract_ref),
        (shift_hbm, shift_ref),
        (speed_hbm, speed_ref),
        (source_hbm, source_in),
    )
    loads = [pltpu.make_async_copy(*pair, load_sem.at[i]) for i, pair in enumerate(pairs)]
    for load in loads:
        load.start()
    barrier = pltpu.get_barrier_semaphore()
    for offset in OFFSETS:
        pl.semaphore_signal(
            barrier, inc=1, device_id={"node": node_at(offset)}, device_id_type=MESH
        )
    for offset in (1, -1):
        pl.semaphore_signal(
            barrier, inc=1, device_id={"freq": band_at(offset)}, device_id_type=MESH
        )

    def parcel(step, group, j):
        piece = pl.ds(j * width, width)
        return pltpu.make_async_remote_copy(
            src_ref=parcel_out.at[step, group, piece],
            dst_ref=parcel_in.at[step, group, piece],
            send_sem=send_sem.at[0],
            recv_sem=recv_sem.at[step, group],
            device_id={"node": node_at(OFFSETS[j])},
            device_id_type=MESH,
        )

    def group_parcels(step, group):
        return pltpu.make_async_remote_copy(
            src_ref=parcel_out.at[step, group],
            dst_ref=parcel_in.at[step, group],
            send_sem=send_sem.at[0],
            recv_sem=recv_sem.at[step, group],
            device_id={"node": node_at(OFFSETS[0])},
            device_id_type=MESH,
        )

    def all_parcels():
        return pltpu.make_async_remote_copy(
            src_ref=parcel_out,
            dst_ref=parcel_in,
            send_sem=send_sem.at[0],
            recv_sem=recv_sem.at[0, 0],
            device_id={"node": node_at(OFFSETS[0])},
            device_id_type=MESH,
        )

    def all_bands():
        return pltpu.make_async_remote_copy(
            src_ref=band_in,
            dst_ref=band_in,
            send_sem=send_sem.at[1],
            recv_sem=band_recv_sem.at[0, 0],
            device_id={"freq": band_at(1)},
            device_id_type=MESH,
        )

    def band_copy(step, side):
        row = (block - edge, 0)[side]
        return pltpu.make_async_remote_copy(
            src_ref=spectra.at[step, (groups - 1, 0)[side], pl.ds(row, edge)],
            dst_ref=band_in.at[step, side],
            send_sem=send_sem.at[1],
            recv_sem=band_recv_sem.at[step, side],
            device_id={"freq": band_at((1, -1)[side])},
            device_id_type=MESH,
        )

    def cut(k):
        return pl.ds(k * TILE, TILE)

    def lhs(group, part, k):
        return lambda: parts[group, part, :, cut(k)]

    def local_jobs(group, entries):
        return [
            [
                (
                    lambda k=k, m=m, unit=unit: pick_local[k, cut(m), cut(unit)],
                    totals[unit][k],
                    lhs(group, 0, m),
                    lhs(group, 1, m),
                )
                for k in entries
                for m in range(local // TILE)
            ]
            for unit in range(2)
        ]

    def halo_jobs(turn_index):
        slot = turn_index % 2
        return [
            [
                (
                    lambda k=k, unit=unit: pick_halo[k, :, cut(unit)],
                    totals[unit][k],
                    lambda: halo_parts[slot, 0],
                    lambda: halo_parts[slot, 1],
                )
                for k in range(degree)
            ]
            for unit in range(2)
        ]

    def select_jobs(group):
        return [
            [
                (
                    lambda unit=unit: select[cut(unit), :],
                    totals[unit][degree],
                    lhs(group, 0, unit),
                    lhs(group, 1, unit),
                )
            ]
            for unit in range(2)
        ]

    def join(*lists):
        return [[job for jobs in lists for job in jobs[unit]] for unit in range(2)]

    def send_group(step, group):
        picked = pltpu.matmul_pop(totals[0][degree]) + pltpu.matmul_pop(totals[1][degree])
        picked = jnp.concatenate([picked, jnp.zeros((128 - block, TILE), F32)], axis=0)
        parcel_out[step, group] = picked.T[:halo]
        for j in reversed(range(len(OFFSETS))):
            parcel(step, group, j).start()

    def send_bands(step, group):
        if group == 0:
            band_copy(step, 1).start()
        if group == groups - 1:
            band_copy(step, 0).start()

    for load in loads[:2]:
        load.wait()
    for unit in range(2):
        for total in totals[unit]:
            pltpu.matmul_pop(total)

    chosen = []
    for offset in OFFSETS:
        target = node_at(offset)
        row = jnp.zeros((1, width), jnp.int32)
        for s in range(slots):
            row = row + jnp.where(nbr_ref[0, s] == target, send_ref[s], 0)
        chosen.append(row)
    fill = jnp.full((1, select.shape[1] - halo), -1, jnp.int32)
    chosen = jnp.concatenate(chosen + [fill], axis=1)
    node_ids = lax.broadcasted_iota(jnp.int32, select.shape, 0)
    select[...] = jnp.where(node_ids == chosen, 1.0, 0.0).astype(BF16)

    def pack(ref, group):
        rows = [ref[group + i * STRIDE] for i in range(members)]
        fill = jnp.zeros((block - members * angles, local), F32)
        return jnp.concatenate(rows + [fill], axis=0)

    for load in loads[3:-1]:
        load.wait()
    adjacency = adjacency_ref[...]
    own = lax.broadcasted_iota(jnp.int32, adjacency.shape, 1)
    used = adjacency != own
    relative = adjacency - local
    slot_of = relative // width
    moved = jnp.zeros_like(adjacency)
    for s in range(slots):
        place = jnp.int32(0)
        for j, offset in enumerate(OFFSETS):
            place = place + jnp.where(nbr_ref[0, s] == node_at(-offset), (j - s) * width, 0)
        moved = moved + jnp.where(slot_of == s, place, 0)
    in_halo = jnp.where(adjacency >= local, relative + moved, -1)
    chunk = 32
    first_ids = lax.broadcasted_iota(jnp.int32, (chunk, local), 0)

    def fill_from(out, target):
        def fill(c, carry):
            at = pl.multiple_of(c * chunk, chunk)
            ids = first_ids + at
            for k in range(degree):
                hit = jnp.where(ids == target[k : k + 1], 1.0, 0.0)
                out[k, pl.ds(at, chunk), :] = hit.astype(BF16)
            return carry

        lax.fori_loop(0, out.shape[1] // chunk, fill, 0)

    fill_from(pick_local, adjacency)
    units = Units(join(*[select_jobs(group) for group in ORDER]))
    pl.semaphore_wait(barrier, len(OFFSETS) + 2)
    loads[2].wait()
    loads[-1].wait()
    for group in ORDER:
        value = pack(old_in, group)
        spectra[0, group] = value
        parts[group, 0], parts[group, 1] = split(value)
        send_bands(0, group)
        units.run(1)
        send_group(0, group)

    fill_from(pick_halo, in_halo)

    period = 2 * angles
    cosine = jnp.broadcast_to(trig_ref[:, 0:1], (period, local))
    sine = jnp.broadcast_to(trig_ref[:, 1:2], (period, local))
    across = jnp.where(used, normals_ref[0], 0.0)
    along = jnp.where(used, normals_ref[1], 0.0)
    outward = jnp.zeros((period, local), F32)
    for k in range(degree):
        flux = cosine * across[k : k + 1] + sine * along[k : k + 1]
        outward = outward + jnp.maximum(flux, 0.0)
        inward = jnp.maximum(-flux, 0.0)
        edge_weight[k, pl.ds(0, period)] = inward
        edge_weight[k, pl.ds(period, block - period)] = inward[: block - period]
    time_weight = weight_ref[...]
    freq_shift = shift_ref[...]
    turning = refract_ref[...] * cosine
    for i, one in enumerate((turning, -turning)):
        one = jnp.maximum(one, 0.0)
        turn[i, pl.ds(0, period)] = one
        turn[i, pl.ds(period, block - period)] = one[: block - period]
    fixed = time_weight + jnp.abs(turning) + jnp.abs(freq_shift)
    outward = jnp.concatenate([outward, outward[: block - period]], axis=0)
    fixed = jnp.concatenate([fixed, fixed[: block - period]], axis=0)
    row_ids = lax.broadcasted_iota(jnp.int32, (block, local), 0)
    for group in ORDER:
        speed = jnp.full((block, local), speed_ref[0, group], F32)
        for i in range(1, members):
            speed = jnp.where(row_ids >= i * angles, speed_ref[0, group + i * STRIDE], speed)
        one = 1.0 / (fixed + speed * outward)
        inverse[group] = one
        speed_inverse[group] = speed * one
        base[group] = (time_weight * spectra[0, group] + pack(source_in, group)) * one

    rising = jnp.maximum(freq_shift, 0.0)
    falling = jnp.maximum(-freq_shift, 0.0)
    half_rows = lax.broadcasted_iota(jnp.int32, (block, TILE), 0)
    is_first = functools.reduce(jnp.logical_or, [half_rows == i * angles for i in range(members)])
    is_last = functools.reduce(
        jnp.logical_or, [half_rows == i * angles + angles - 1 for i in range(members)]
    )
    gap = jnp.zeros((angles, TILE), F32)
    tail = jnp.zeros((block - members * angles, TILE), F32)
    edge_rows = lax.broadcasted_iota(jnp.int32, (edge, TILE), 0)

    def gathered(unit):
        total = None
        for k in range(degree):
            term = edge_weight[k, :, cut(unit)] * pltpu.matmul_pop(totals[unit][k])
            total = term if total is None else total + term
        return total

    def prepare(step, group, unit):
        columns = cut(unit)
        value = spectra[step, group, :, columns]
        before = jnp.where(
            is_first, pltpu.roll(value, block - angles + 1, 0), pltpu.roll(value, 1, 0)
        )
        after = jnp.where(
            is_last, pltpu.roll(value, angles - 1, 0), pltpu.roll(value, block - 1, 0)
        )
        if group > 0:
            below = spectra[step, group - 1, :, columns]
        else:
            moved = spectra[step, groups - 1, :, columns]
            below = jnp.concatenate([gap, moved[: (members - 1) * angles], tail], axis=0)
        if group < groups - 1:
            above = spectra[step, group + 1, :, columns]
        else:
            moved = spectra[step, 0, :, columns]
            above = jnp.concatenate([moved[angles : members * angles], gap, tail], axis=0)
        inflow = turn[0, :, columns] * before + turn[1, :, columns] * after
        inflow = inflow + rising[:, unit * TILE : (unit + 1) * TILE] * below
        inflow = inflow + falling[:, unit * TILE : (unit + 1) * TILE] * above
        ready[group, :, columns] = base[group, :, columns] + inflow * inverse[group, :, columns]

    def finish(step, group, unit):
        columns = cut(unit)
        value = ready[group, :, columns]
        value = value + speed_inverse[group, :, columns] * gathered(unit)
        if group == 0:
            rim = band_in[step, 0, :, columns] * rising[:, unit * TILE : (unit + 1) * TILE]
            rim = rim * inverse[group, pl.ds(0, edge), columns]
            rim = jnp.where(jnp.logical_and(edge_rows < angles, band_me > 0), rim, 0.0)
            value = jnp.concatenate([value[:edge] + rim, value[edge:]], axis=0)
        if group == groups - 1:
            rim = band_in[step, 1, :, columns] * falling[:, unit * TILE : (unit + 1) * TILE]
            rim = rim * inverse[group, pl.ds(block - edge, edge), columns]
            rim = jnp.where(
                jnp.logical_and(edge_rows < angles, band_me < freq_count - 1), rim, 0.0
            )
            value = jnp.concatenate(
                [value[: block - edge], value[block - edge :] + rim], axis=0
            )
        if step == ITERS - 1:
            for i in range(members):
                out_ref[group + i * STRIDE, :, columns] = value[i * angles : (i + 1) * angles]
        else:
            spectra[step + 1, group, :, columns] = value
            high, low = split(value)
            parts[group, 0, :, columns] = high
            parts[group, 1, :, columns] = low

    def arrive(step, index):
        group = ORDER[index]
        group_parcels(step, group).wait_recv()
        arrived = parcel_in[step, group].T[:block]
        arrived = jnp.concatenate([arrived, jnp.zeros((block, TILE - halo), F32)], axis=1)
        halo_parts[index % 2, 0], halo_parts[index % 2, 1] = split(arrived)

    def arrive_band(step, group):
        if group == 0:
            band_copy(step, 0).wait_recv()
        if group == groups - 1:
            band_copy(step, 1).wait_recv()

    first = ORDER[0]
    plan = [local_jobs(first, range(FILL))]
    for step in range(ITERS):
        plan.append(local_jobs(first, range(FILL, degree)))
        for group in ORDER[1:]:
            plan.append(local_jobs(group, range(degree)))
        for index, group in enumerate(ORDER):
            plan.append(halo_jobs(index))
            if step + 1 < ITERS:
                if index + 1 == len(ORDER):
                    plan.append(local_jobs(first, range(FILL)))
                plan.append(select_jobs(group))
    units = Units(join(*plan))
    per_entry = local // TILE
    units.run(FILL * per_entry)
    for step in range(ITERS):
        for group in ORDER:
            for unit in range(2):
                prepare(step, group, unit)
        units.run((degree - FILL) * per_entry)
        for group in ORDER:
            if group != first:
                units.run(degree * per_entry)
            for unit in range(2):
                columns = cut(unit)
                local_part = speed_inverse[group, :, columns] * gathered(unit)
                ready[group, :, columns] = ready[group, :, columns] + local_part
        arrive(step, 0)
        for index, group in enumerate(ORDER):
            units.run(degree)
            arrive_band(step, group)
            for unit in range(2):
                finish(step, group, unit)
            if step + 1 < ITERS:
                send_bands(step + 1, group)
            if index + 1 < len(ORDER):
                arrive(step, index + 1)
            elif step + 1 < ITERS:
                units.run(FILL * per_entry)
            if step + 1 < ITERS:
                units.run(1)
                send_group(step + 1, group)

    all_parcels().wait_send()
    all_bands().wait_send()


def body(
    node_count,
    freq_count,
    action_old,
    source,
    time_weight,
    group_speed,
    normals,
    refract,
    freq_shift,
    nbr_list,
    send_nodes,
    adjacency,
):
    bands, angles, local = action_old.shape
    degree = adjacency.shape[0]
    slots, width = send_nodes.shape[1:]
    groups = STRIDE
    members = bands // groups
    block = -(-members * angles // 16) * 16
    edge = -(-angles // 8) * 8
    halo = slots * width
    theta = 2.0 * math.pi * (np.arange(2 * angles) % angles) / angles
    trig = np.zeros((2 * angles, 128), np.float32)
    trig[:, 0] = np.cos(theta)
    trig[:, 1] = np.sin(theta)
    vmem = pl.BlockSpec(memory_space=pltpu.VMEM)
    anywhere = pl.BlockSpec(memory_space=pl.ANY)
    dma = pltpu.SemaphoreType.DMA
    return pl.pallas_call(
        functools.partial(kernel, node_count, freq_count),
        out_shape=pltpu.VMEM(action_old.shape, F32),
        in_specs=[anywhere] * 11,
        out_specs=vmem,
        scratch_shapes=[
            pltpu.VMEM((bands, angles, local), F32),
            pltpu.VMEM((bands, angles, local), F32),
            pltpu.VMEM((ITERS, groups, block, local), F32),
            pltpu.VMEM((groups, block, local), F32),
            pltpu.VMEM((groups, block, local), F32),
            pltpu.VMEM((groups, block, local), F32),
            pltpu.VMEM((degree, block, local), F32),
            pltpu.VMEM((2, block, local), F32),
            pltpu.VMEM((degree, local, local), BF16),
            pltpu.VMEM((degree, TILE, local), BF16),
            pltpu.VMEM((local, TILE), BF16),
            pltpu.VMEM((groups, 2, block, local), BF16),
            pltpu.VMEM((2, 2, block, TILE), BF16),
            pltpu.VMEM((groups, block, local), F32),
            pltpu.VMEM((ITERS, groups, halo, 128), F32),
            pltpu.VMEM((ITERS, groups, halo, 128), F32),
            pltpu.VMEM((ITERS, 2, edge, local), F32),
            pltpu.VMEM((1, local), F32),
            pltpu.VMEM((1, local), F32),
            pltpu.VMEM((1, local), F32),
            pltpu.SMEM((1, bands), F32),
            pltpu.VMEM((2, degree, local), F32),
            pltpu.SMEM((1, slots), jnp.int32),
            pltpu.VMEM((slots, 1, width), jnp.int32),
            pltpu.VMEM((degree, local), jnp.int32),
            pltpu.VMEM((2 * angles, 128), F32),
            dma((11,)),
            dma((2,)),
            dma((ITERS, groups)),
            dma((ITERS, 2)),
        ],
        compiler_params=pltpu.CompilerParams(
            collective_id=0, has_side_effects=True, vmem_limit_bytes=VMEM_LIMIT
        ),
    )(
        action_old,
        source,
        time_weight[None, :],
        refract[None, :],
        freq_shift[None, :],
        group_speed[None, :],
        normals,
        nbr_list,
        send_nodes.reshape(slots, 1, width),
        adjacency,
        jnp.asarray(trig),
    )


def solution(mesh):
    in_specs = (
        P("freq", None, "node"),
        P("freq", None, "node"),
        P("node"),
        P("freq"),
        P(None, None, "node"),
        P("node"),
        P("node"),
        P("node", None),
        P("node", None, None),
        P(None, "node"),
    )
    return jax.shard_map(
        functools.partial(body, mesh.shape["node"], mesh.shape["freq"]),
        mesh=mesh,
        in_specs=in_specs,
        out_specs=P("freq", None, "node"),
        check_vma=False,
    )
```

```python
import functools
import math

import jax
import jax.numpy as jnp
import numpy as np
from jax import lax
from jax.experimental import pallas as pl
from jax.experimental.pallas import tpu as pltpu
from jax.sharding import PartitionSpec as P

REACH = 3
ITERS = 3
MESH = pl.DeviceIdType.MESH
F32 = jnp.float32
BF16 = jnp.bfloat16
OFFSETS = tuple(sign * reach for reach in range(1, REACH + 1) for sign in (1, -1))
STRIDE = 3
ORDER = (0, 2, 1)
TILE = 256
FILL = 4
VMEM_LIMIT = 66100000


def split(value):
    high = value.astype(BF16)
    low = (value - high.astype(F32)).astype(BF16)
    return high, low


class Units:
    def __init__(self, jobs):
        self.jobs = jobs
        self.at = [0, 0]
        for unit in range(2):
            self.stage(unit, 0)

    def stage(self, unit, index):
        if index < len(self.jobs[unit]):
            matrix = self.jobs[unit][index][0]()
            pltpu.matmul_push_rhs(matrix, staging_register=index % 2, mxu_index=unit)

    def run(self, count):
        for _ in range(count):
            for unit in range(2):
                index = self.at[unit]
                self.stage(unit, index + 1)
                _, total, high, low = self.jobs[unit][index]
                pltpu.matmul_acc_lhs(total, high(), load_staged_rhs=index % 2)
                pltpu.matmul_acc_lhs(total, low())
                self.at[unit] = index + 1


def kernel(node_count, freq_count, *refs):
    degree = refs[9].shape[0]
    block = refs[14].shape[2]
    count = degree + 1
    specs = [pltpu.ACC(unit)((block, TILE), F32) for unit in range(2) for _ in range(count)]

    def scoped(*totals):
        run(node_count, freq_count, (totals[:count], totals[count:]), *refs)

    pl.run_scoped(scoped, *specs)


def run(
    node_count,
    freq_count,
    totals,
    old_hbm,
    source_hbm,
    weight_hbm,
    refract_hbm,
    shift_hbm,
    speed_hbm,
    normals_hbm,
    nbr_hbm,
    send_hbm,
    adjacency_hbm,
    trig_hbm,
    out_ref,
    old_in,
    source_in,
    spectra,
    base,
    inverse,
    speed_inverse,
    edge_weight,
    turn,
    pick_local,
    pick_halo,
    select,
    parts,
    halo_parts,
    ready,
    parcel_out,
    parcel_in,
    band_in,
    weight_ref,
    refract_ref,
    shift_ref,
    speed_ref,
    normals_ref,
    nbr_ref,
    send_ref,
    adjacency_ref,
    trig_ref,
    load_sem,
    send_sem,
    recv_sem,
    band_recv_sem,
):
    bands, angles, local = old_in.shape
    groups, block = spectra.shape[1:3]
    edge = band_in.shape[2]
    degree = adjacency_ref.shape[0]
    slots, _, width = send_ref.shape
    halo = slots * width
    members = bands // groups
    me = lax.axis_index("node")
    band_me = lax.axis_index("freq")

    def node_at(offset):
        return lax.rem(me + offset + node_count, node_count)

    def band_at(offset):
        return lax.rem(band_me + offset + freq_count, freq_count)

    pairs = (
        (nbr_hbm, nbr_ref),
        (send_hbm, send_ref),
        (old_hbm, old_in),
        (adjacency_hbm, adjacency_ref),
        (normals_hbm, normals_ref),
        (trig_hbm, trig_ref),
        (weight_hbm, weight_ref),
        (refract_hbm, refract_ref),
        (shift_hbm, shift_ref),
        (speed_hbm, speed_ref),
        (source_hbm, source_in),
    )
    loads = [pltpu.make_async_copy(*pair, load_sem.at[i]) for i, pair in enumerate(pairs)]
    for load in loads:
        load.start()
    barrier = pltpu.get_barrier_semaphore()
    for offset in OFFSETS:
        pl.semaphore_signal(
            barrier, inc=1, device_id={"node": node_at(offset)}, device_id_type=MESH
        )
    for offset in (1, -1):
        pl.semaphore_signal(
            barrier, inc=1, device_id={"freq": band_at(offset)}, device_id_type=MESH
        )

    def parcel(step, group, j):
        piece = pl.ds(j * width, width)
        return pltpu.make_async_remote_copy(
            src_ref=parcel_out.at[step, group, piece],
            dst_ref=parcel_in.at[step, group, piece],
            send_sem=send_sem.at[0],
            recv_sem=recv_sem.at[step, group],
            device_id={"node": node_at(OFFSETS[j])},
            device_id_type=MESH,
        )

    def group_parcels(step, group):
        return pltpu.make_async_remote_copy(
            src_ref=parcel_out.at[step, group],
            dst_ref=parcel_in.at[step, group],
            send_sem=send_sem.at[0],
            recv_sem=recv_sem.at[step, group],
            device_id={"node": node_at(OFFSETS[0])},
            device_id_type=MESH,
        )

    def all_parcels():
        return pltpu.make_async_remote_copy(
            src_ref=parcel_out,
            dst_ref=parcel_in,
            send_sem=send_sem.at[0],
            recv_sem=recv_sem.at[0, 0],
            device_id={"node": node_at(OFFSETS[0])},
            device_id_type=MESH,
        )

    def all_bands():
        return pltpu.make_async_remote_copy(
            src_ref=band_in,
            dst_ref=band_in,
            send_sem=send_sem.at[1],
            recv_sem=band_recv_sem.at[0, 0],
            device_id={"freq": band_at(1)},
            device_id_type=MESH,
        )

    def band_copy(step, side):
        row = (block - edge, 0)[side]
        return pltpu.make_async_remote_copy(
            src_ref=spectra.at[step, (groups - 1, 0)[side], pl.ds(row, edge)],
            dst_ref=band_in.at[step, side],
            send_sem=send_sem.at[1],
            recv_sem=band_recv_sem.at[step, side],
            device_id={"freq": band_at((1, -1)[side])},
            device_id_type=MESH,
        )

    def cut(k):
        return pl.ds(k * TILE, TILE)

    def lhs(group, part, k):
        return lambda: parts[group, part, :, cut(k)]

    def local_jobs(group, entries):
        return [
            [
                (
                    lambda k=k, m=m, unit=unit: pick_local[k, cut(m), cut(unit)],
                    totals[unit][k],
                    lhs(group, 0, m),
                    lhs(group, 1, m),
                )
                for k in entries
                for m in range(local // TILE)
            ]
            for unit in range(2)
        ]

    def halo_jobs(turn_index):
        slot = turn_index % 2
        return [
            [
                (
                    lambda k=k, unit=unit: pick_halo[k, :, cut(unit)],
                    totals[unit][k],
                    lambda: halo_parts[slot, 0],
                    lambda: halo_parts[slot, 1],
                )
                for k in range(degree)
            ]
            for unit in range(2)
        ]

    def select_jobs(group):
        return [
            [
                (
                    lambda unit=unit: select[cut(unit), :],
                    totals[unit][degree],
                    lhs(group, 0, unit),
                    lhs(group, 1, unit),
                )
            ]
            for unit in range(2)
        ]

    def join(*lists):
        return [[job for jobs in lists for job in jobs[unit]] for unit in range(2)]

    def pick_group(step, group):
        picked = pltpu.matmul_pop(totals[0][degree]) + pltpu.matmul_pop(totals[1][degree])
        picked = jnp.concatenate([picked, jnp.zeros((128 - block, TILE), F32)], axis=0)
        parcel_out[step, group] = picked.T[:halo]

    def start_group(step, group):
        for j in reversed(range(len(OFFSETS))):
            parcel(step, group, j).start()

    def send_group(step, group):
        pick_group(step, group)
        start_group(step, group)

    def send_bands(step, group):
        if group == 0:
            band_copy(step, 1).start()
        if group == groups - 1:
            band_copy(step, 0).start()

    for load in loads[:2]:
        load.wait()
    for unit in range(2):
        for total in totals[unit]:
            pltpu.matmul_pop(total)

    chosen = []
    for offset in OFFSETS:
        target = node_at(offset)
        row = jnp.zeros((1, width), jnp.int32)
        for s in range(slots):
            row = row + jnp.where(nbr_ref[0, s] == target, send_ref[s], 0)
        chosen.append(row)
    fill = jnp.full((1, select.shape[1] - halo), -1, jnp.int32)
    chosen = jnp.concatenate(chosen + [fill], axis=1)
    node_ids = lax.broadcasted_iota(jnp.int32, select.shape, 0)
    select[...] = jnp.where(node_ids == chosen, 1.0, 0.0).astype(BF16)

    def pack(ref, group):
        rows = [ref[group + i * STRIDE] for i in range(members)]
        fill = jnp.zeros((block - members * angles, local), F32)
        return jnp.concatenate(rows + [fill], axis=0)

    for load in loads[3:-1]:
        load.wait()
    adjacency = adjacency_ref[...]
    own = lax.broadcasted_iota(jnp.int32, adjacency.shape, 1)
    used = adjacency != own
    relative = adjacency - local
    slot_of = relative // width
    moved = jnp.zeros_like(adjacency)
    for s in range(slots):
        place = jnp.int32(0)
        for j, offset in enumerate(OFFSETS):
            place = place + jnp.where(nbr_ref[0, s] == node_at(-offset), (j - s) * width, 0)
        moved = moved + jnp.where(slot_of == s, place, 0)
    in_halo = jnp.where(adjacency >= local, relative + moved, -1)
    chunk = 32
    first_ids = lax.broadcasted_iota(jnp.int32, (chunk, local), 0)

    def fill_from(out, target):
        def fill(c, carry):
            at = pl.multiple_of(c * chunk, chunk)
            ids = first_ids + at
            for k in range(degree):
                hit = jnp.where(ids == target[k : k + 1], 1.0, 0.0)
                out[k, pl.ds(at, chunk), :] = hit.astype(BF16)
            return carry

        lax.fori_loop(0, out.shape[1] // chunk, fill, 0)

    fill_from(pick_local, adjacency)
    units = Units(join(*[select_jobs(group) for group in ORDER]))
    loads[2].wait()
    loads[-1].wait()
    for group in ORDER:
        value = pack(old_in, group)
        spectra[0, group] = value
        parts[group, 0], parts[group, 1] = split(value)
        units.run(1)
        pick_group(0, group)
        if group == ORDER[0]:
            pl.semaphore_wait(barrier, len(OFFSETS) + 2)
        send_bands(0, group)
        start_group(0, group)

    fill_from(pick_halo, in_halo)

    period = 2 * angles
    cosine = jnp.broadcast_to(trig_ref[:, 0:1], (period, local))
    sine = jnp.broadcast_to(trig_ref[:, 1:2], (period, local))
    across = jnp.where(used, normals_ref[0], 0.0)
    along = jnp.where(used, normals_ref[1], 0.0)
    outward = jnp.zeros((period, local), F32)
    for k in range(degree):
        flux = cosine * across[k : k + 1] + sine * along[k : k + 1]
        outward = outward + jnp.maximum(flux, 0.0)
        inward = jnp.maximum(-flux, 0.0)
        edge_weight[k, pl.ds(0, period)] = inward
        edge_weight[k, pl.ds(period, block - period)] = inward[: block - period]
    time_weight = weight_ref[...]
    freq_shift = shift_ref[...]
    turning = refract_ref[...] * cosine
    for i, one in enumerate((turning, -turning)):
        one = jnp.maximum(one, 0.0)
        turn[i, pl.ds(0, period)] = one
        turn[i, pl.ds(period, block - period)] = one[: block - period]
    fixed = time_weight + jnp.abs(turning) + jnp.abs(freq_shift)
    outward = jnp.concatenate([outward, outward[: block - period]], axis=0)
    fixed = jnp.concatenate([fixed, fixed[: block - period]], axis=0)
    row_ids = lax.broadcasted_iota(jnp.int32, (block, local), 0)
    for group in ORDER:
        speed = jnp.full((block, local), speed_ref[0, group], F32)
        for i in range(1, members):
            speed = jnp.where(row_ids >= i * angles, speed_ref[0, group + i * STRIDE], speed)
        one = 1.0 / (fixed + speed * outward)
        inverse[group] = one
        speed_inverse[group] = speed * one
        base[group] = (time_weight * spectra[0, group] + pack(source_in, group)) * one

    rising = jnp.maximum(freq_shift, 0.0)
    falling = jnp.maximum(-freq_shift, 0.0)
    half_rows = lax.broadcasted_iota(jnp.int32, (block, TILE), 0)
    is_first = functools.reduce(jnp.logical_or, [half_rows == i * angles for i in range(members)])
    is_last = functools.reduce(
        jnp.logical_or, [half_rows == i * angles + angles - 1 for i in range(members)]
    )
    gap = jnp.zeros((angles, TILE), F32)
    tail = jnp.zeros((block - members * angles, TILE), F32)
    edge_rows = lax.broadcasted_iota(jnp.int32, (edge, TILE), 0)

    def gathered(unit):
        total = None
        for k in range(degree):
            term = edge_weight[k, :, cut(unit)] * pltpu.matmul_pop(totals[unit][k])
            total = term if total is None else total + term
        return total

    def prepare(step, group, unit):
        columns = cut(unit)
        value = spectra[step, group, :, columns]
        before = jnp.where(
            is_first, pltpu.roll(value, block - angles + 1, 0), pltpu.roll(value, 1, 0)
        )
        after = jnp.where(
            is_last, pltpu.roll(value, angles - 1, 0), pltpu.roll(value, block - 1, 0)
        )
        if group > 0:
            below = spectra[step, group - 1, :, columns]
        else:
            moved = spectra[step, groups - 1, :, columns]
            below = jnp.concatenate([gap, moved[: (members - 1) * angles], tail], axis=0)
        if group < groups - 1:
            above = spectra[step, group + 1, :, columns]
        else:
            moved = spectra[step, 0, :, columns]
            above = jnp.concatenate([moved[angles : members * angles], gap, tail], axis=0)
        inflow = turn[0, :, columns] * before + turn[1, :, columns] * after
        inflow = inflow + rising[:, unit * TILE : (unit + 1) * TILE] * below
        inflow = inflow + falling[:, unit * TILE : (unit + 1) * TILE] * above
        ready[group, :, columns] = base[group, :, columns] + inflow * inverse[group, :, columns]

    def finish(step, group, unit):
        columns = cut(unit)
        value = ready[group, :, columns]
        value = value + speed_inverse[group, :, columns] * gathered(unit)
        if group == 0:
            rim = band_in[step, 0, :, columns] * rising[:, unit * TILE : (unit + 1) * TILE]
            rim = rim * inverse[group, pl.ds(0, edge), columns]
            rim = jnp.where(jnp.logical_and(edge_rows < angles, band_me > 0), rim, 0.0)
            value = jnp.concatenate([value[:edge] + rim, value[edge:]], axis=0)
        if group == groups - 1:
            rim = band_in[step, 1, :, columns] * falling[:, unit * TILE : (unit + 1) * TILE]
            rim = rim * inverse[group, pl.ds(block - edge, edge), columns]
            rim = jnp.where(
                jnp.logical_and(edge_rows < angles, band_me < freq_count - 1), rim, 0.0
            )
            value = jnp.concatenate(
                [value[: block - edge], value[block - edge :] + rim], axis=0
            )
        if step == ITERS - 1:
            for i in range(members):
                out_ref[group + i * STRIDE, :, columns] = value[i * angles : (i + 1) * angles]
        else:
            spectra[step + 1, group, :, columns] = value
            high, low = split(value)
            parts[group, 0, :, columns] = high
            parts[group, 1, :, columns] = low

    def arrive(step, index):
        group = ORDER[index]
        group_parcels(step, group).wait_recv()
        arrived = parcel_in[step, group].T[:block]
        arrived = jnp.concatenate([arrived, jnp.zeros((block, TILE - halo), F32)], axis=1)
        halo_parts[index % 2, 0], halo_parts[index % 2, 1] = split(arrived)

    def arrive_band(step, group):
        if group == 0:
            band_copy(step, 0).wait_recv()
        if group == groups - 1:
            band_copy(step, 1).wait_recv()

    first = ORDER[0]
    plan = [local_jobs(first, range(FILL))]
    for step in range(ITERS):
        plan.append(local_jobs(first, range(FILL, degree)))
        for group in ORDER[1:]:
            plan.append(local_jobs(group, range(degree)))
        for index, group in enumerate(ORDER):
            plan.append(halo_jobs(index))
            if step + 1 < ITERS:
                if index + 1 == len(ORDER):
                    plan.append(local_jobs(first, range(FILL)))
                plan.append(select_jobs(group))
    units = Units(join(*plan))
    per_entry = local // TILE
    units.run(FILL * per_entry)
    for step in range(ITERS):
        for group in ORDER:
            for unit in range(2):
                prepare(step, group, unit)
        units.run((degree - FILL) * per_entry)
        for group in ORDER:
            if group != first:
                units.run(degree * per_entry)
            for unit in range(2):
                columns = cut(unit)
                local_part = speed_inverse[group, :, columns] * gathered(unit)
                ready[group, :, columns] = ready[group, :, columns] + local_part
        arrive(step, 0)
        for index, group in enumerate(ORDER):
            units.run(degree)
            arrive_band(step, group)
            for unit in range(2):
                finish(step, group, unit)
            if step + 1 < ITERS:
                send_bands(step + 1, group)
            if index + 1 < len(ORDER):
                arrive(step, index + 1)
            elif step + 1 < ITERS:
                units.run(FILL * per_entry)
            if step + 1 < ITERS:
                units.run(1)
                send_group(step + 1, group)

    all_parcels().wait_send()
    all_bands().wait_send()


def body(
    node_count,
    freq_count,
    action_old,
    source,
    time_weight,
    group_speed,
    normals,
    refract,
    freq_shift,
    nbr_list,
    send_nodes,
    adjacency,
):
    bands, angles, local = action_old.shape
    degree = adjacency.shape[0]
    slots, width = send_nodes.shape[1:]
    groups = STRIDE
    members = bands // groups
    block = -(-members * angles // 16) * 16
    edge = -(-angles // 8) * 8
    halo = slots * width
    theta = 2.0 * math.pi * (np.arange(2 * angles) % angles) / angles
    trig = np.zeros((2 * angles, 128), np.float32)
    trig[:, 0] = np.cos(theta)
    trig[:, 1] = np.sin(theta)
    vmem = pl.BlockSpec(memory_space=pltpu.VMEM)
    anywhere = pl.BlockSpec(memory_space=pl.ANY)
    dma = pltpu.SemaphoreType.DMA
    return pl.pallas_call(
        functools.partial(kernel, node_count, freq_count),
        out_shape=pltpu.VMEM(action_old.shape, F32),
        in_specs=[anywhere] * 11,
        out_specs=vmem,
        scratch_shapes=[
            pltpu.VMEM((bands, angles, local), F32),
            pltpu.VMEM((bands, angles, local), F32),
            pltpu.VMEM((ITERS, groups, block, local), F32),
            pltpu.VMEM((groups, block, local), F32),
            pltpu.VMEM((groups, block, local), F32),
            pltpu.VMEM((groups, block, local), F32),
            pltpu.VMEM((degree, block, local), F32),
            pltpu.VMEM((2, block, local), F32),
            pltpu.VMEM((degree, local, local), BF16),
            pltpu.VMEM((degree, TILE, local), BF16),
            pltpu.VMEM((local, TILE), BF16),
            pltpu.VMEM((groups, 2, block, local), BF16),
            pltpu.VMEM((2, 2, block, TILE), BF16),
            pltpu.VMEM((groups, block, local), F32),
            pltpu.VMEM((ITERS, groups, halo, 128), F32),
            pltpu.VMEM((ITERS, groups, halo, 128), F32),
            pltpu.VMEM((ITERS, 2, edge, local), F32),
            pltpu.VMEM((1, local), F32),
            pltpu.VMEM((1, local), F32),
            pltpu.VMEM((1, local), F32),
            pltpu.SMEM((1, bands), F32),
            pltpu.VMEM((2, degree, local), F32),
            pltpu.SMEM((1, slots), jnp.int32),
            pltpu.VMEM((slots, 1, width), jnp.int32),
            pltpu.VMEM((degree, local), jnp.int32),
            pltpu.VMEM((2 * angles, 128), F32),
            dma((11,)),
            dma((2,)),
            dma((ITERS, groups)),
            dma((ITERS, 2)),
        ],
        compiler_params=pltpu.CompilerParams(
            collective_id=0, has_side_effects=True, vmem_limit_bytes=VMEM_LIMIT
        ),
    )(
        action_old,
        source,
        time_weight[None, :],
        refract[None, :],
        freq_shift[None, :],
        group_speed[None, :],
        normals,
        nbr_list,
        send_nodes.reshape(slots, 1, width),
        adjacency,
        jnp.asarray(trig),
    )


def solution(mesh):
    in_specs = (
        P("freq", None, "node"),
        P("freq", None, "node"),
        P("node"),
        P("freq"),
        P(None, None, "node"),
        P("node"),
        P("node"),
        P("node", None),
        P("node", None, None),
        P(None, "node"),
    )
    return jax.shard_map(
        functools.partial(body, mesh.shape["node"], mesh.shape["freq"]),
        mesh=mesh,
        in_specs=in_specs,
        out_specs=P("freq", None, "node"),
        check_vma=False,
    )
```
